1024 devices in a mesh: ffn: 64 (over z, core), mp: 16 (over y, x).
Axes of the slice: x: 4, y: 4, z: 32, core: 2. Of those that a mesh axis runs over, the one named last changes fastest.
Arguments:
- hidden_in: bfloat16 [256, 8192], P(None, 'mp'), may hold values from -40 to 40
- norm_gain: float32 [8192], P('mp'), may hold values from 0.1 to 1.9
- grad_out: bfloat16 [256, 8192], P(None, 'mp'), may hold values from -6 to 6
- gate_weight: bfloat16 [8192, 28672], P('mp', 'ffn'), may hold values from -0.0625 to 0.0625
- up_weight: bfloat16 [8192, 28672], P('mp', 'ffn'), may hold values from -0.0625 to 0.0625
- down_weight: bfloat16 [28672, 8192], P('ffn', 'mp'), may hold values from -0.03125 to 0.03125
Outputs:
- grad_hidden: bfloat16 [256, 8192], P(None, 'mp')
- grad_gain: float32 [8192], P('mp')
- grad_gate: bfloat16 [8192, 28672], P('mp', 'ffn')
- grad_up: bfloat16 [8192, 28672], P('mp', 'ffn')
- grad_down: bfloat16 [28672, 8192], P('ffn', 'mp')
The draws below stay inside these ranges and needn't reach their ends.
All inputs are finite; a program needn't handle non-finite values.
Results may differ from the reference program's by a relative error of at most 0.0066.
Values may be sent and summed in bfloat16 or wider, within the bound.
No kernel may reach another device: no remote copies, remote signals or barrier semaphores. Data moves between devices by JAX's collectives and lax.ppermute only.
A program may use at most 32 MiB of HBM per device.

```python
import math
import jax
import jax.numpy as jnp
from jax import lax

D = 8192
FF = 28672
TOKENS = 256


def draw_hidden_in(key, part):
    keys = jax.random.split(jax.random.fold_in(key, 17), 3)
    row_scale = jnp.exp(jax.random.uniform(keys[0], (TOKENS, 1), jnp.float32) * math.log(10.0))
    ramp = jnp.linspace(0.0, math.log(3.0), D, dtype=jnp.float32)
    col_scale = jnp.exp(jax.random.uniform(keys[1], (1, D), jnp.float32) * 0.5 * math.log(10.0) + ramp[None, :])
    base = jax.random.normal(keys[2], (TOKENS, D), jnp.float32)
    base = jnp.clip(base, -4.0, 4.0)
    return (base * row_scale * col_scale / 10.0).astype(jnp.bfloat16)


def levels(key, shape, shards, low, high):
    def one(dim, parts):
        heights = jax.random.uniform(jax.random.fold_in(jax.random.fold_in(key, 6), dim), (parts,), jnp.float32, low / len(shards), high / len(shards))
        return jnp.repeat(jnp.exp(heights), shape[dim] // parts).reshape((-1,) + (1,) * (len(shape) - dim - 1))

    gain = one(*shards[0])
    for cut in shards[1:]:
        gain = gain * one(*cut)
    return gain


def scatter_about(key, extent, width, most, shards=(), kind=jnp.bfloat16):
    result = jax.random.normal(key, extent, jnp.float32) * width
    if len(shards) > 0:
        result = levels(key, extent, shards, -0.22, 0.18) * result
    return jnp.clip(result, min=-most, max=most).astype(kind)


def setup_inputs(seed: int = 0) -> dict:
    streams_of = jax.random.split(jax.random.key(seed), 7)
    return {
        "hidden_in": draw_hidden_in(jax.random.fold_in(streams_of[6], 71), 0),
        "norm_gain": jnp.clip(1.0 + 0.18 * jax.random.normal(streams_of[1], (D,), jnp.float32), 0.1, 1.9),
        "grad_out": scatter_about(streams_of[2], (TOKENS, D), 1.0, 6.0, ((1, 16),)),
        "gate_weight": scatter_about(streams_of[3], (D, FF), D ** -0.5, 0.0625, ((0, 16), (1, 64))),
        "up_weight": scatter_about(streams_of[4], (D, FF), D ** -0.5, 0.0625, ((0, 16), (1, 64))),
        "down_weight": scatter_about(streams_of[5], (FF, D), FF ** -0.5, 0.03125, ((0, 64), (1, 16))),
    }


epsilon = 1e-05

def reference(hidden_in, norm_gain, grad_out, gate_weight, up_weight, down_weight):
    hidden = hidden_in.astype(jnp.float32)
    inverse = lax.rsqrt(lax.optimization_barrier(jnp.sum(hidden * hidden, axis=1)) / D + epsilon)
    scaled = (hidden * norm_gain).astype(jnp.bfloat16)
    gate = inverse[:, None] * jnp.dot(scaled, gate_weight, preferred_element_type=jnp.float32)
    up_val = inverse[:, None] * jnp.dot(scaled, up_weight, preferred_element_type=jnp.float32)
    sigma = jax.nn.sigmoid(gate)
    activation = (gate * sigma * up_val).astype(jnp.bfloat16)
    act_grad = jnp.dot(grad_out, down_weight.T, preferred_element_type=jnp.float32)
    grad_down = jnp.dot(activation.T, grad_out, preferred_element_type=jnp.float32).astype(jnp.bfloat16)
    gate_grad = (inverse[:, None] * act_grad * up_val * sigma * (1.0 + gate * (1.0 - sigma))).astype(jnp.bfloat16)
    up_grad = (inverse[:, None] * act_grad * gate * sigma).astype(jnp.bfloat16)
    grad_gate = jnp.dot(scaled.T, gate_grad, preferred_element_type=jnp.float32).astype(jnp.bfloat16)
    grad_up = jnp.dot(scaled.T, up_grad, preferred_element_type=jnp.float32).astype(jnp.bfloat16)
    input_grad = jnp.dot(gate_grad, gate_weight.T, preferred_element_type=jnp.float32) + jnp.dot(up_grad, up_weight.T, preferred_element_type=jnp.float32)
    products = lax.optimization_barrier(jnp.sum(norm_gain * hidden * input_grad, axis=1))
    grad_hidden = (norm_gain * input_grad - hidden * (inverse * inverse * products / D)[:, None]).astype(jnp.bfloat16)
    grad_gain = lax.optimization_barrier(jnp.sum(hidden * input_grad, axis=0))
    return (grad_hidden, grad_gain, grad_gate, grad_up, grad_down)
```

```python
import jax
import jax.numpy as jnp
from jax import lax
from jax.sharding import PartitionSpec as P

D = 8192
epsilon = 1e-05
RING = 8


def two_terms(x):
    high = lax.reduce_precision(x, 8, 7)
    return high.astype(jnp.bfloat16), (x - high).astype(jnp.bfloat16)


def units_by_tokens(weight, acts, weight_dim):
    return lax.dot_general(
        weight, acts, (((weight_dim,), (1,)), ((), ())), preferred_element_type=jnp.float32
    )


def body(hidden_in, norm_gain, grad_out, gate_weight, up_weight, down_weight):
    f32, bf16 = jnp.float32, jnp.bfloat16
    tokens, width = hidden_in.shape
    units = gate_weight.shape[1]
    mp, ffn = lax.axis_size("mp"), lax.axis_size("ffn")
    ublocks, thalf = mp // 2, tokens // 2
    ub = units // ublocks
    levels = ffn // 2 // RING
    me = lax.axis_index("ffn")
    core, z = me % 2, me // 2

    hidden = hidden_in.astype(f32)
    scaled = (hidden * norm_gain).astype(bf16)
    squared = jnp.sum(hidden * hidden, axis=1)

    gate_t = units_by_tokens(gate_weight, scaled, 0)
    up_t = units_by_tokens(up_weight, scaled, 0)
    down_t = units_by_tokens(down_weight, grad_out, 1)

    def cut(x):
        return x.astype(bf16).reshape(ublocks, ub, 2, thalf).transpose(0, 2, 1, 3)

    def extra_rows(high, low):
        rows = jnp.concatenate(
            [high.reshape(2, 1, thalf), low.reshape(2, 1, thalf), jnp.zeros((2, 6, thalf), bf16)], axis=1
        )
        return rows

    square_rows = jnp.broadcast_to(extra_rows(*two_terms(squared))[None], (ublocks, 2, 8, thalf))
    send = jnp.concatenate([cut(gate_t), cut(up_t), cut(down_t), square_rows], axis=2)
    send = send.reshape(mp, 3 * ub + 8, thalf)
    got = jnp.sum(lax.all_to_all(send, "mp", 0, 0, tiled=True).astype(f32), axis=0)

    square_sum = got[3 * ub] + got[3 * ub + 1]
    inverse = lax.rsqrt(square_sum / D + epsilon)
    gate = inverse * got[:ub]
    up_val = inverse * got[ub : 2 * ub]
    act_grad = got[2 * ub : 3 * ub]
    sigma = jax.nn.sigmoid(gate)
    activation = (gate * sigma * up_val).astype(bf16)
    gate_grad = (inverse * act_grad * up_val * sigma * (1.0 + gate * (1.0 - sigma))).astype(bf16)
    up_grad = (inverse * act_grad * gate * sigma).astype(bf16)
    pulled = inverse * jnp.sum(gate_grad.astype(f32) * gate + up_grad.astype(f32) * up_val, axis=0) / D
    high, low = two_terms(pulled)
    piece = jnp.concatenate(
        [activation, gate_grad, up_grad, high[None], low[None], jnp.zeros((6, thalf), bf16)], axis=0
    )
    everything = lax.all_to_all(jnp.broadcast_to(piece, (mp, *piece.shape)), "mp", 0, 0, tiled=True)
    everything = everything.reshape(ublocks, 2, 3 * ub + 8, thalf)

    def joined(k):
        part = everything[:, :, k * ub : (k + 1) * ub]
        return part.transpose(0, 2, 1, 3).reshape(units, tokens)

    act_t, gate_grad_t, up_grad_t = joined(0), joined(1), joined(2)
    pulled = jnp.sum(everything[:, :, 3 * ub : 3 * ub + 2].astype(f32), axis=(0, 2)).reshape(tokens)

    input_part = lax.dot_general(
        gate_grad_t, gate_weight, (((0,), (1,)), ((), ())), preferred_element_type=f32
    ) + lax.dot_general(up_grad_t, up_weight, (((0,), (1,)), ((), ())), preferred_element_type=f32)

    lanes = width // 128
    pulled_rows = tokens // 128

    def vector_rows(x):
        rows = [t.reshape(-1, 128) for t in two_terms(x)]
        used = rows[0].shape[0] * 2
        return jnp.concatenate(rows + [jnp.zeros((-used % 8, 128), bf16)] * (used % 8 > 0), axis=0)

    def rows_vector(rows, count):
        return rows[..., : count // 128, :].astype(f32) + rows[..., count // 128 : count // 64, :].astype(f32)

    halves = input_part.reshape(2, thalf, lanes, 128).transpose(0, 2, 1, 3)
    mine = lax.dynamic_index_in_dim(halves, core, 0, keepdims=False)
    other = lax.dynamic_index_in_dim(halves, 1 - core, 0, keepdims=False)
    pair = [(i, i ^ 1) for i in range(ffn)]
    packed = jnp.concatenate([other.astype(bf16).reshape(-1, 128), vector_rows(pulled)], axis=0)
    came = lax.ppermute(packed, "ffn", pair)
    body_rows = thalf * lanes
    half_sum = mine + came[:body_rows].astype(f32).reshape(lanes, thalf, 128)
    pulled = pulled.reshape(-1, 128) + rows_vector(came[body_rows:], tokens)

    share = thalf // RING
    near = [[(g * RING + j) * 2 + c for j in range(RING)] for g in range(levels) for c in range(2)]
    cuts = half_sum.astype(bf16).reshape(lanes, RING, share, 128).transpose(1, 0, 2, 3)
    cuts = cuts.reshape(RING, share * lanes, 128)
    extra = vector_rows(pulled.reshape(-1))
    cuts = jnp.concatenate([cuts, jnp.broadcast_to(extra, (RING, *extra.shape))], axis=1)
    came = lax.all_to_all(cuts, "ffn", 0, 0, tiled=True, axis_index_groups=near)
    summed = jnp.sum(came[:, : share * lanes].astype(f32), axis=0)
    pulled = jnp.sum(rows_vector(came[:, share * lanes :], tokens), axis=0)

    packed = jnp.concatenate([summed.astype(bf16), vector_rows(pulled.reshape(-1))], axis=0)
    nz = ffn // 2

    def shifted(x, k):
        return lax.ppermute(x, "ffn", [(i, (i // 2 + k * RING) % nz * 2 + i % 2) for i in range(ffn)])

    far = [packed] + [shifted(packed, k) for k in range(1, levels)]
    while len(far) > 1:
        half = len(far) // 2
        far = [a.astype(f32) + b.astype(f32) for a, b in zip(far[:half], far[half:])]
    total = far[0]
    input_grad = total[: share * lanes].reshape(lanes, share, 128)
    pulled = rows_vector(total[share * lanes :], tokens).reshape(tokens)

    first = core * thalf + z % RING * share
    rows_hidden = lax.dynamic_slice_in_dim(hidden_in, first, share, 0).astype(f32)
    rows_hidden = rows_hidden.reshape(share, lanes, 128).transpose(1, 0, 2)
    rows_pulled = lax.dynamic_slice_in_dim(pulled, first, share, 0)
    gain = norm_gain.reshape(lanes, 1, 128)
    rows_out = (gain * input_grad - rows_hidden * rows_pulled[None, :, None]).astype(bf16)
    gain_part = jnp.sum(rows_hidden * input_grad, axis=1)
    piece = jnp.concatenate([rows_out.reshape(-1, 128), vector_rows(gain_part.reshape(-1))], axis=0)

    near_rows = lax.all_to_all(
        jnp.broadcast_to(piece, (RING, *piece.shape)), "ffn", 0, 0, tiled=True, axis_index_groups=near
    )
    pair_rows = lax.ppermute(near_rows, "ffn", pair)
    first_half = jnp.where(core == 0, near_rows, pair_rows)
    second_half = jnp.where(core == 0, pair_rows, near_rows)
    both = jnp.stack([first_half, second_half])
    rows = both[:, :, : share * lanes].reshape(2, RING, lanes, share, 128)
    grad_hidden = rows.transpose(0, 1, 3, 2, 4).reshape(tokens, width)
    grad_gain = jnp.sum(rows_vector(both[:, :, share * lanes :], width), axis=(0, 1)).reshape(width)

    def weight_grad(lhs, rhs, dims):
        return lax.dot_general(lhs, rhs, (dims, ((), ())), preferred_element_type=f32).astype(bf16)

    grad_down = weight_grad(act_t, grad_out, ((1,), (0,)))
    grad_gate = weight_grad(scaled, gate_grad_t, ((0,), (1,)))
    grad_up = weight_grad(scaled, up_grad_t, ((0,), (1,)))
    return (grad_hidden, grad_gain, grad_gate, grad_up, grad_down)


def solution(mesh):
    placed = (P(None, "mp"), P("mp"), P(None, "mp"), P("mp", "ffn"), P("mp", "ffn"), P("ffn", "mp"))
    return jax.shard_map(
        body,
        mesh=mesh,
        in_specs=placed,
        out_specs=(P(None, "mp"), P("mp"), P("mp", "ffn"), P("mp", "ffn"), P("ffn", "mp")),
        check_vma=False,
    )
```

```python
import jax
import jax.numpy as jnp
from jax import lax
from jax.sharding import PartitionSpec as P

D = 8192
epsilon = 1e-05
RING = 8


def two_terms(x):
    high = lax.reduce_precision(x, 8, 7)
    return high.astype(jnp.bfloat16), (x - high).astype(jnp.bfloat16)


def units_by_tokens(weight, acts, weight_dim):
    return lax.dot_general(
        weight, acts, (((weight_dim,), (1,)), ((), ())), preferred_element_type=jnp.float32
    )


def body(hidden_in, norm_gain, grad_out, gate_weight, up_weight, down_weight):
    f32, bf16 = jnp.float32, jnp.bfloat16
    tokens, width = hidden_in.shape
    units = gate_weight.shape[1]
    mp, ffn = lax.axis_size("mp"), lax.axis_size("ffn")
    ublocks, thalf = mp // 2, tokens // 2
    ub = units // ublocks
    levels = ffn // 2 // RING
    me = lax.axis_index("ffn")
    core, z = me % 2, me // 2

    hidden = hidden_in.astype(f32)
    scaled = (hidden * norm_gain).astype(bf16)
    squared = jnp.sum(hidden * hidden, axis=1)

    gate_t = units_by_tokens(gate_weight, scaled, 0)
    up_t = units_by_tokens(up_weight, scaled, 0)
    down_t = units_by_tokens(down_weight, grad_out, 1)

    def cut(x):
        return x.astype(bf16).reshape(ublocks, ub, 2, thalf).transpose(0, 2, 1, 3)

    def extra_rows(high, low):
        rows = jnp.concatenate(
            [high.reshape(2, 1, thalf), low.reshape(2, 1, thalf), jnp.zeros((2, 6, thalf), bf16)], axis=1
        )
        return rows

    square_rows = jnp.broadcast_to(extra_rows(*two_terms(squared))[None], (ublocks, 2, 8, thalf))
    send = jnp.concatenate([cut(gate_t), cut(up_t), cut(down_t), square_rows], axis=2)
    send = send.reshape(mp, 3 * ub + 8, thalf)
    got = jnp.sum(lax.all_to_all(send, "mp", 0, 0, tiled=True).astype(f32), axis=0)

    square_sum = got[3 * ub] + got[3 * ub + 1]
    inverse = lax.rsqrt(square_sum / D + epsilon)
    gate = inverse * got[:ub]
    up_val = inverse * got[ub : 2 * ub]
    act_grad = got[2 * ub : 3 * ub]
    sigma = jax.nn.sigmoid(gate)
    activation = (gate * sigma * up_val).astype(bf16)
    gate_grad = (inverse * act_grad * up_val * sigma * (1.0 + gate * (1.0 - sigma))).astype(bf16)
    up_grad = (inverse * act_grad * gate * sigma).astype(bf16)
    pulled = inverse * jnp.sum(gate_grad.astype(f32) * gate + up_grad.astype(f32) * up_val, axis=0) / D
    high, low = two_terms(pulled)
    piece = jnp.concatenate(
        [activation, gate_grad, up_grad, high[None], low[None], jnp.zeros((6, thalf), bf16)], axis=0
    )
    everything = lax.all_to_all(jnp.broadcast_to(piece, (mp, *piece.shape)), "mp", 0, 0, tiled=True)
    everything = everything.reshape(ublocks, 2, 3 * ub + 8, thalf)

    def joined(k):
        part = everything[:, :, k * ub : (k + 1) * ub]
        return part.transpose(0, 2, 1, 3).reshape(units, tokens)

    act_t, gate_grad_t, up_grad_t = joined(0), joined(1), joined(2)
    pulled = jnp.sum(everything[:, :, 3 * ub : 3 * ub + 2].astype(f32), axis=(0, 2)).reshape(tokens)

    input_part = lax.dot_general(
        gate_grad_t, gate_weight, (((0,), (1,)), ((), ())), preferred_element_type=f32
    ) + lax.dot_general(up_grad_t, up_weight, (((0,), (1,)), ((), ())), preferred_element_type=f32)

    lanes = width // 128
    pulled_rows = tokens // 128

    def vector_rows(x):
        rows = [t.reshape(-1, 128) for t in two_terms(x)]
        used = rows[0].shape[0] * 2
        return jnp.concatenate(rows + [jnp.zeros((-used % 8, 128), bf16)] * (used % 8 > 0), axis=0)

    def rows_vector(rows, count):
        return rows[..., : count // 128, :].astype(f32) + rows[..., count // 128 : count // 64, :].astype(f32)

    halves = input_part.reshape(2, thalf, lanes, 128).transpose(0, 2, 1, 3)
    mine = lax.dynamic_index_in_dim(halves, core, 0, keepdims=False)
    other = lax.dynamic_index_in_dim(halves, 1 - core, 0, keepdims=False)
    pair = [(i, i ^ 1) for i in range(ffn)]
    packed = jnp.concatenate([other.astype(bf16).reshape(-1, 128), vector_rows(pulled)], axis=0)
    came = lax.ppermute(packed, "ffn", pair)
    body_rows = thalf * lanes
    half_sum = mine + came[:body_rows].astype(f32).reshape(lanes, thalf, 128)
    pulled = pulled.reshape(-1, 128) + rows_vector(came[body_rows:], tokens)

    share = thalf // RING
    near = [[(g * RING + j) * 2 + c for j in range(RING)] for g in range(levels) for c in range(2)]
    cuts = half_sum.astype(bf16).reshape(lanes, RING, share, 128).transpose(1, 0, 2, 3)
    cuts = cuts.reshape(RING, share * lanes, 128)
    extra = vector_rows(pulled.reshape(-1))
    cuts = jnp.concatenate([cuts, jnp.broadcast_to(extra, (RING, *extra.shape))], axis=1)
    came = lax.all_to_all(cuts, "ffn", 0, 0, tiled=True, axis_index_groups=near)
    summed = jnp.sum(came[:, : share * lanes].astype(f32), axis=0)
    pulled = jnp.sum(rows_vector(came[:, share * lanes :], tokens), axis=0)

    packed = jnp.concatenate([summed, pulled.reshape(-1, 128), jnp.zeros((8 - pulled_rows, 128), f32)], axis=0)
    owners = [[(k * RING + j) * 2 + c for k in range(levels)] for j in range(RING) for c in range(2)]
    total = jnp.sum(
        lax.all_to_all(
            jnp.broadcast_to(packed, (levels, *packed.shape)), "ffn", 0, 0, tiled=True, axis_index_groups=owners
        ),
        axis=0,
    )
    input_grad = total[: share * lanes].reshape(lanes, share, 128)
    pulled = total[share * lanes : share * lanes + pulled_rows].reshape(tokens)

    first = core * thalf + z % RING * share
    rows_hidden = lax.dynamic_slice_in_dim(hidden_in, first, share, 0).astype(f32)
    rows_hidden = rows_hidden.reshape(share, lanes, 128).transpose(1, 0, 2)
    rows_pulled = lax.dynamic_slice_in_dim(pulled, first, share, 0)
    gain = norm_gain.reshape(lanes, 1, 128)
    rows_out = (gain * input_grad - rows_hidden * rows_pulled[None, :, None]).astype(bf16)
    gain_part = jnp.sum(rows_hidden * input_grad, axis=1)
    piece = jnp.concatenate([rows_out.reshape(-1, 128), vector_rows(gain_part.reshape(-1))], axis=0)

    near_rows = lax.all_to_all(
        jnp.broadcast_to(piece, (RING, *piece.shape)), "ffn", 0, 0, tiled=True, axis_index_groups=near
    )
    pair_rows = lax.ppermute(near_rows, "ffn", pair)
    first_half = jnp.where(core == 0, near_rows, pair_rows)
    second_half = jnp.where(core == 0, pair_rows, near_rows)
    both = jnp.stack([first_half, second_half])
    rows = both[:, :, : share * lanes].reshape(2, RING, lanes, share, 128)
    grad_hidden = rows.transpose(0, 1, 3, 2, 4).reshape(tokens, width)
    grad_gain = jnp.sum(rows_vector(both[:, :, share * lanes :], width), axis=(0, 1)).reshape(width)

    def weight_grad(lhs, rhs, dims):
        return lax.dot_general(lhs, rhs, (dims, ((), ())), preferred_element_type=f32).astype(bf16)

    grad_down = weight_grad(act_t, grad_out, ((1,), (0,)))
    grad_gate = weight_grad(scaled, gate_grad_t, ((0,), (1,)))
    grad_up = weight_grad(scaled, up_grad_t, ((0,), (1,)))
    return (grad_hidden, grad_gain, grad_gate, grad_up, grad_down)


def solution(mesh):
    placed = (P(None, "mp"), P("mp"), P(None, "mp"), P("mp", "ffn"), P("mp", "ffn"), P("ffn", "mp"))
    return jax.shard_map(
        body,
        mesh=mesh,
        in_specs=placed,
        out_specs=(P(None, "mp"), P("mp"), P("mp", "ffn"), P("mp", "ffn"), P("ffn", "mp")),
        check_vma=False,
    )
```

```python
import jax
import jax.numpy as jnp
from jax import lax
from jax.sharding import PartitionSpec as P

D = 8192
epsilon = 1e-05
RING = 8


def two_terms(x):
    high = lax.reduce_precision(x, 8, 7)
    return high.astype(jnp.bfloat16), (x - high).astype(jnp.bfloat16)


def units_by_tokens(weight, acts, weight_dim):
    return lax.dot_general(
        weight, acts, (((weight_dim,), (1,)), ((), ())), preferred_element_type=jnp.float32
    )


def body(hidden_in, norm_gain, grad_out, gate_weight, up_weight, down_weight):
    f32, bf16 = jnp.float32, jnp.bfloat16
    tokens, width = hidden_in.shape
    units = gate_weight.shape[1]
    mp, ffn = lax.axis_size("mp"), lax.axis_size("ffn")
    ublocks, thalf = mp // 2, tokens // 2
    ub = units // ublocks
    levels = ffn // 2 // RING
    me = lax.axis_index("ffn")
    core, z = me % 2, me // 2

    hidden = hidden_in.astype(f32)
    scaled = (hidden * norm_gain).astype(bf16)
    squared = jnp.sum(hidden * hidden, axis=1)

    gate_t = units_by_tokens(gate_weight, scaled, 0)
    up_t = units_by_tokens(up_weight, scaled, 0)
    down_t = units_by_tokens(down_weight, grad_out, 1)

    def cut(x):
        return x.astype(bf16).reshape(ublocks, ub, 2, thalf).transpose(0, 2, 1, 3)

    def extra_rows(high, low):
        rows = jnp.concatenate(
            [high.reshape(2, 1, thalf), low.reshape(2, 1, thalf), jnp.zeros((2, 6, thalf), bf16)], axis=1
        )
        return rows

    square_rows = jnp.broadcast_to(extra_rows(*two_terms(squared))[None], (ublocks, 2, 8, thalf))
    send = jnp.concatenate([cut(gate_t), cut(up_t), cut(down_t), square_rows], axis=2)
    send = send.reshape(mp, 3 * ub + 8, thalf)
    got = jnp.sum(lax.all_to_all(send, "mp", 0, 0, tiled=True).astype(f32), axis=0)

    square_sum = got[3 * ub] + got[3 * ub + 1]
    inverse = lax.rsqrt(square_sum / D + epsilon)
    gate = inverse * got[:ub]
    up_val = inverse * got[ub : 2 * ub]
    act_grad = got[2 * ub : 3 * ub]
    sigma = jax.nn.sigmoid(gate)
    activation = (gate * sigma * up_val).astype(bf16)
    gate_grad = (inverse * act_grad * up_val * sigma * (1.0 + gate * (1.0 - sigma))).astype(bf16)
    up_grad = (inverse * act_grad * gate * sigma).astype(bf16)
    pulled = inverse * jnp.sum(gate_grad.astype(f32) * gate + up_grad.astype(f32) * up_val, axis=0) / D
    high, low = two_terms(pulled)
    piece = jnp.concatenate(
        [activation, gate_grad, up_grad, high[None], low[None], jnp.zeros((6, thalf), bf16)], axis=0
    )
    everything = lax.all_to_all(jnp.broadcast_to(piece, (mp, *piece.shape)), "mp", 0, 0, tiled=True)
    everything = everything.reshape(ublocks, 2, 3 * ub + 8, thalf)

    def joined(k):
        part = everything[:, :, k * ub : (k + 1) * ub]
        return part.transpose(0, 2, 1, 3).reshape(units, tokens)

    act_t, gate_grad_t, up_grad_t = joined(0), joined(1), joined(2)
    pulled = jnp.sum(everything[:, :, 3 * ub : 3 * ub + 2].astype(f32), axis=(0, 2)).reshape(tokens)

    input_part = lax.dot_general(
        gate_grad_t, gate_weight, (((0,), (1,)), ((), ())), preferred_element_type=f32
    ) + lax.dot_general(up_grad_t, up_weight, (((0,), (1,)), ((), ())), preferred_element_type=f32)

    lanes = width // 128
    pulled_rows = tokens // 128

    def vector_rows(x):
        rows = [t.reshape(-1, 128) for t in two_terms(x)]
        used = rows[0].shape[0] * 2
        return jnp.concatenate(rows + [jnp.zeros((-used % 8, 128), bf16)] * (used % 8 > 0), axis=0)

    def rows_vector(rows, count):
        return rows[..., : count // 128, :].astype(f32) + rows[..., count // 128 : count // 64, :].astype(f32)

    halves = input_part.reshape(2, thalf, lanes, 128).transpose(0, 2, 1, 3)
    mine = lax.dynamic_index_in_dim(halves, core, 0, keepdims=False)
    other = lax.dynamic_index_in_dim(halves, 1 - core, 0, keepdims=False)
    pair = [(i, i ^ 1) for i in range(ffn)]
    packed = jnp.concatenate([other.astype(bf16).reshape(-1, 128), vector_rows(pulled)], axis=0)
    came = lax.ppermute(packed, "ffn", pair)
    body_rows = thalf * lanes
    half_sum = mine + came[:body_rows].astype(f32).reshape(lanes, thalf, 128)
    pulled = pulled.reshape(-1, 128) + rows_vector(came[body_rows:], tokens)

    share = thalf // RING
    near = [[(g * RING + j) * 2 + c for j in range(RING)] for g in range(levels) for c in range(2)]
    cuts = half_sum.astype(bf16).reshape(lanes, RING, share, 128).transpose(1, 0, 2, 3)
    cuts = cuts.reshape(RING, share * lanes, 128)
    extra = vector_rows(pulled.reshape(-1))
    cuts = jnp.concatenate([cuts, jnp.broadcast_to(extra, (RING, *extra.shape))], axis=1)
    came = lax.all_to_all(cuts, "ffn", 0, 0, tiled=True, axis_index_groups=near)
    summed = jnp.sum(came[:, : share * lanes].astype(f32), axis=0)
    pulled = jnp.sum(rows_vector(came[:, share * lanes :], tokens), axis=0)

    packed = jnp.concatenate([summed, pulled.reshape(-1, 128), jnp.zeros((8 - pulled_rows, 128), f32)], axis=0)
    owners = [[(k * RING + j) * 2 + c for k in range(levels)] for j in range(RING) for c in range(2)]
    total = jnp.sum(lax.all_gather(packed, "ffn", axis_index_groups=owners), axis=0)
    input_grad = total[: share * lanes].reshape(lanes, share, 128)
    pulled = total[share * lanes : share * lanes + pulled_rows].reshape(tokens)

    first = core * thalf + z % RING * share
    rows_hidden = lax.dynamic_slice_in_dim(hidden_in, first, share, 0).astype(f32)
    rows_hidden = rows_hidden.reshape(share, lanes, 128).transpose(1, 0, 2)
    rows_pulled = lax.dynamic_slice_in_dim(pulled, first, share, 0)
    gain = norm_gain.reshape(lanes, 1, 128)
    rows_out = (gain * input_grad - rows_hidden * rows_pulled[None, :, None]).astype(bf16)
    gain_part = jnp.sum(rows_hidden * input_grad, axis=1)
    piece = jnp.concatenate([rows_out.reshape(-1, 128), vector_rows(gain_part.reshape(-1))], axis=0)

    near_rows = lax.all_to_all(
        jnp.broadcast_to(piece, (RING, *piece.shape)), "ffn", 0, 0, tiled=True, axis_index_groups=near
    )
    pair_rows = lax.ppermute(near_rows, "ffn", pair)
    first_half = jnp.where(core == 0, near_rows, pair_rows)
    second_half = jnp.where(core == 0, pair_rows, near_rows)
    both = jnp.stack([first_half, second_half])
    rows = both[:, :, : share * lanes].reshape(2, RING, lanes, share, 128)
    grad_hidden = rows.transpose(0, 1, 3, 2, 4).reshape(tokens, width)
    grad_gain = jnp.sum(rows_vector(both[:, :, share * lanes :], width), axis=(0, 1)).reshape(width)

    def weight_grad(lhs, rhs, dims):
        return lax.dot_general(lhs, rhs, (dims, ((), ())), preferred_element_type=f32).astype(bf16)

    grad_down = weight_grad(act_t, grad_out, ((1,), (0,)))
    grad_gate = weight_grad(scaled, gate_grad_t, ((0,), (1,)))
    grad_up = weight_grad(scaled, up_grad_t, ((0,), (1,)))
    return (grad_hidden, grad_gain, grad_gate, grad_up, grad_down)


def solution(mesh):
    placed = (P(None, "mp"), P("mp"), P(None, "mp"), P("mp", "ffn"), P("mp", "ffn"), P("ffn", "mp"))
    return jax.shard_map(
        body,
        mesh=mesh,
        in_specs=placed,
        out_specs=(P(None, "mp"), P("mp"), P("mp", "ffn"), P("mp", "ffn"), P("ffn", "mp")),
        check_vma=False,
    )
```

```python
import jax
import jax.numpy as jnp
from jax import lax
from jax.experimental import pallas as pl
from jax.experimental.pallas import tpu as pltpu
from jax.sharding import PartitionSpec as P

D = 8192
epsilon = 1e-05
RING = 8


def two_terms(x):
    high = lax.reduce_precision(x, 8, 7)
    return high.astype(jnp.bfloat16), (x - high).astype(jnp.bfloat16)


def in_vmem(x):
    return pltpu.with_memory_space_constraint(x, pltpu.VMEM)


def split_terms(x):
    high = x.astype(jnp.bfloat16)
    return high, (x - high.astype(jnp.float32)).astype(jnp.bfloat16)


def across(lhs, rhs):
    return lax.dot_general(lhs, rhs, (((1,), (1,)), ((), ())), preferred_element_type=jnp.float32)


def partial_kernel(
    hidden_hbm, gain_ref, gate_hbm, up_hbm, grad_hbm, down_hbm, send_ref, gate, up, hidden, grad, down, sems
):
    moves = [
        pltpu.make_async_copy(source, target, sems.at[i])
        for i, (source, target) in enumerate(
            ((hidden_hbm, hidden), (grad_hbm, grad), (down_hbm, down), (gate_hbm, gate), (up_hbm, up))
        )
    ]
    for move in moves:
        move.start()
    pieces, rows, lanes = send_ref.shape
    units = gate.shape[0]
    ub = units * 2 // pieces

    def pack(part, first):
        for u in range(pieces // 2):
            for half in range(2):
                send_ref[2 * u + half, first : first + ub, :] = part[
                    u * ub : (u + 1) * ub, half * lanes : (half + 1) * lanes
                ].astype(jnp.bfloat16)

    moves[0].wait()
    wide = hidden[...].astype(jnp.float32)
    scaled = (wide * gain_ref[...]).astype(jnp.bfloat16)
    high, low = split_terms(wide * wide)
    ones = jnp.ones((8, hidden.shape[1]), jnp.bfloat16)
    squared = across(ones, high) + across(ones, low)
    high, low = split_terms(squared)
    row = lax.broadcasted_iota(jnp.int32, squared.shape, 0)
    extra = jnp.where(row == 0, high.astype(jnp.float32), jnp.where(row == 1, low.astype(jnp.float32), 0.0))
    for piece in range(pieces):
        half = piece % 2
        send_ref[piece, 3 * ub : rows, :] = extra[:, half * lanes : (half + 1) * lanes].astype(jnp.bfloat16)
    moves[1].wait()
    moves[2].wait()
    pack(across(down[...], grad[...]), 2 * ub)
    moves[3].wait()
    pack(across(gate[...], scaled), 0)
    moves[4].wait()
    pack(across(up[...], scaled), ub)


def partials(hidden_in, norm_gain, gate_rows, up_rows, grad_out, down_weight, pieces):
    tokens, width = hidden_in.shape
    units = gate_rows.shape[0]
    anywhere = pl.BlockSpec(memory_space=pl.ANY)
    inside = pl.BlockSpec(memory_space=pltpu.VMEM)
    return pl.pallas_call(
        partial_kernel,
        out_shape=(
            pltpu.VMEM((pieces, 3 * (units * 2 // pieces) + 8, tokens // 2), jnp.bfloat16),
            pltpu.VMEM((units, width), jnp.bfloat16),
            pltpu.VMEM((units, width), jnp.bfloat16),
        ),
        in_specs=[anywhere, inside, anywhere, anywhere, anywhere, anywhere],
        out_specs=(inside,) * 3,
        scratch_shapes=[
            pltpu.VMEM((tokens, width), jnp.bfloat16),
            pltpu.VMEM((tokens, width), jnp.bfloat16),
            pltpu.VMEM((units, width), jnp.bfloat16),
            pltpu.SemaphoreType.DMA((5,)),
        ],
        name="partials",
    )(hidden_in, norm_gain.reshape(1, width), gate_rows, up_rows, grad_out, down_weight)


def piece_kernel(came_ref, out_ref):
    pieces, rows, lanes = came_ref.shape
    ub = (rows - 8) // 3
    got = came_ref[0].astype(jnp.float32)
    for i in range(1, pieces):
        got = got + came_ref[i].astype(jnp.float32)
    square_sum = got[3 * ub : 3 * ub + 1] + got[3 * ub + 1 : 3 * ub + 2]
    inverse = lax.rsqrt(square_sum / D + epsilon)
    gate = inverse * got[:ub]
    up_val = inverse * got[ub : 2 * ub]
    act_grad = got[2 * ub : 3 * ub]
    sigma = jax.nn.sigmoid(gate)
    activation = (gate * sigma * up_val).astype(jnp.bfloat16)
    gate_grad = (inverse * act_grad * up_val * sigma * (1.0 + gate * (1.0 - sigma))).astype(jnp.bfloat16)
    up_grad = (inverse * act_grad * gate * sigma).astype(jnp.bfloat16)
    both = gate_grad.astype(jnp.float32) * gate + up_grad.astype(jnp.float32) * up_val
    pulled = jnp.broadcast_to(inverse * jnp.sum(both, axis=0, keepdims=True) / D, (8, lanes))
    high, low = split_terms(pulled)
    row = lax.broadcasted_iota(jnp.int32, (8, lanes), 0)
    extra = jnp.where(row == 0, high.astype(jnp.float32), jnp.where(row == 1, low.astype(jnp.float32), 0.0))
    extra = extra.astype(jnp.bfloat16)
    for i in range(pieces):
        out_ref[i, :ub, :] = activation
        out_ref[i, ub : 2 * ub, :] = gate_grad
        out_ref[i, 2 * ub : 3 * ub, :] = up_grad
        out_ref[i, 3 * ub :, :] = extra


def finish_kernel(core_ref, near_ref, pair_ref, rows_ref, gain_ref):
    ring, rows, lane = near_ref.shape
    lanes = rows_ref.shape[1] // lane
    share = (rows - 2 * lanes) // lanes
    first = core_ref[0] == 0
    total = jnp.zeros((lanes, lane), jnp.float32)
    for half in range(2):
        take_near = first if half == 0 else jnp.logical_not(first)
        for k in range(ring):
            got = jnp.where(take_near, near_ref[k].astype(jnp.float32), pair_ref[k].astype(jnp.float32))
            at = (half * ring + k) * share
            for l in range(lanes):
                rows_ref[at : at + share, l * lane : (l + 1) * lane] = got[l * share : (l + 1) * share].astype(jnp.bfloat16)
            total = total + (got[lanes * share : lanes * share + lanes] + got[lanes * share + lanes :])
    gain_ref[...] = total


def body(hidden_in, norm_gain, grad_out, gate_weight, up_weight, down_weight):
    f32, bf16 = jnp.float32, jnp.bfloat16
    tokens, width = hidden_in.shape
    units = gate_weight.shape[1]
    mp, ffn = lax.axis_size("mp"), lax.axis_size("ffn")
    ublocks, thalf = mp // 2, tokens // 2
    ub = units // ublocks
    levels = ffn // 2 // RING
    me = lax.axis_index("ffn")
    core, z = me % 2, me // 2

    send, gate_rows, up_rows = partials(
        hidden_in, norm_gain, gate_weight.T, up_weight.T, grad_out, down_weight, mp
    )
    scaled = (hidden_in.astype(f32) * norm_gain).astype(bf16)
    came = lax.all_to_all(send, "mp", 0, 0, tiled=True)
    piece = pl.pallas_call(
        piece_kernel, out_shape=pltpu.VMEM(came.shape, bf16), name="piece"
    )(in_vmem(came))
    everything = lax.all_to_all(piece, "mp", 0, 0, tiled=True)
    everything = everything.reshape(ublocks, 2, 3 * ub + 8, thalf)

    def joined(k):
        part = everything[:, :, k * ub : (k + 1) * ub]
        return part.transpose(0, 2, 1, 3).reshape(units, tokens)

    act_t, gate_grad_t, up_grad_t = joined(0), joined(1), joined(2)
    pulled = jnp.sum(everything[:, :, 3 * ub : 3 * ub + 2].astype(f32), axis=(0, 2)).reshape(tokens)

    input_part = lax.dot_general(
        gate_grad_t, gate_rows, (((0,), (0,)), ((), ())), preferred_element_type=f32
    ) + lax.dot_general(up_grad_t, up_rows, (((0,), (0,)), ((), ())), preferred_element_type=f32)

    lanes = width // 128
    pulled_rows = tokens // 128

    def vector_rows(x):
        rows = [t.reshape(-1, 128) for t in two_terms(x)]
        used = rows[0].shape[0] * 2
        return jnp.concatenate(rows + [jnp.zeros((-used % 8, 128), bf16)] * (used % 8 > 0), axis=0)

    def rows_vector(rows, count):
        return rows[..., : count // 128, :].astype(f32) + rows[..., count // 128 : count // 64, :].astype(f32)

    halves = input_part.reshape(2, thalf, lanes, 128).transpose(0, 2, 1, 3)
    mine = lax.dynamic_index_in_dim(halves, core, 0, keepdims=False)
    other = lax.dynamic_index_in_dim(halves, 1 - core, 0, keepdims=False)
    pair = [(i, i ^ 1) for i in range(ffn)]
    packed = jnp.concatenate([other.astype(bf16).reshape(-1, 128), vector_rows(pulled)], axis=0)
    came = lax.ppermute(packed, "ffn", pair)
    body_rows = thalf * lanes
    half_sum = mine + came[:body_rows].astype(f32).reshape(lanes, thalf, 128)
    pulled = pulled.reshape(-1, 128) + rows_vector(came[body_rows:], tokens)

    share = thalf // RING
    near = [[(g * RING + j) * 2 + c for j in range(RING)] for g in range(levels) for c in range(2)]
    cuts = half_sum.astype(bf16).reshape(lanes, RING, share, 128).transpose(1, 0, 2, 3)
    cuts = cuts.reshape(RING, share * lanes, 128)
    extra = vector_rows(pulled.reshape(-1))
    cuts = jnp.concatenate([cuts, jnp.broadcast_to(extra, (RING, *extra.shape))], axis=1)
    came = lax.all_to_all(cuts, "ffn", 0, 0, tiled=True, axis_index_groups=near)
    summed = jnp.sum(came[:, : share * lanes].astype(f32), axis=0)
    pulled = jnp.sum(rows_vector(came[:, share * lanes :], tokens), axis=0)

    packed = jnp.concatenate([summed, pulled.reshape(-1, 128), jnp.zeros((8 - pulled_rows, 128), f32)], axis=0)
    owners = [[(k * RING + j) * 2 + c for k in range(levels)] for j in range(RING) for c in range(2)]
    total = jnp.sum(lax.all_gather(packed, "ffn", axis_index_groups=owners), axis=0)
    input_grad = total[: share * lanes].reshape(lanes, share, 128)
    pulled = total[share * lanes : share * lanes + pulled_rows].reshape(tokens)

    first = core * thalf + z % RING * share
    rows_hidden = lax.dynamic_slice_in_dim(hidden_in, first, share, 0).astype(f32)
    rows_hidden = rows_hidden.reshape(share, lanes, 128).transpose(1, 0, 2)
    rows_pulled = lax.dynamic_slice_in_dim(pulled, first, share, 0)
    gain = norm_gain.reshape(lanes, 1, 128)
    rows_out = (gain * input_grad - rows_hidden * rows_pulled[None, :, None]).astype(bf16)
    gain_part = jnp.sum(rows_hidden * input_grad, axis=1)
    piece = jnp.concatenate([rows_out.reshape(-1, 128), vector_rows(gain_part.reshape(-1))], axis=0)

    near_rows = lax.all_to_all(
        jnp.broadcast_to(piece, (RING, *piece.shape)), "ffn", 0, 0, tiled=True, axis_index_groups=near
    )
    pair_rows = lax.ppermute(near_rows, "ffn", pair)
    inside = pl.BlockSpec(memory_space=pltpu.VMEM)
    grad_hidden, grad_gain = pl.pallas_call(
        finish_kernel,
        out_shape=(jax.ShapeDtypeStruct((tokens, width), bf16), jax.ShapeDtypeStruct((lanes, 128), f32)),
        in_specs=[pl.BlockSpec(memory_space=pltpu.SMEM), inside, inside],
        out_specs=(inside, inside),
        name="finish",
    )(core.reshape(1), in_vmem(near_rows), in_vmem(pair_rows))
    grad_gain = grad_gain.reshape(width)

    def weight_grad(lhs, rhs, dims):
        return lax.dot_general(lhs, rhs, (dims, ((), ())), preferred_element_type=f32).astype(bf16)

    grad_down = weight_grad(act_t, grad_out, ((1,), (0,)))
    grad_gate = weight_grad(scaled, gate_grad_t, ((0,), (1,)))
    grad_up = weight_grad(scaled, up_grad_t, ((0,), (1,)))
    return (grad_hidden, grad_gain, grad_gate, grad_up, grad_down)


def solution(mesh):
    placed = (P(None, "mp"), P("mp"), P(None, "mp"), P("mp", "ffn"), P("mp", "ffn"), P("ffn", "mp"))
    return jax.shard_map(
        body,
        mesh=mesh,
        in_specs=placed,
        out_specs=(P(None, "mp"), P("mp"), P("mp", "ffn"), P("mp", "ffn"), P("ffn", "mp")),
        check_vma=False,
    )
```

```python
import jax
import jax.numpy as jnp
from jax import lax
from jax.experimental import pallas as pl
from jax.experimental.pallas import tpu as pltpu
from jax.sharding import PartitionSpec as P

D = 8192
epsilon = 1e-05
RING = 8


def in_vmem(x):
    return pltpu.with_memory_space_constraint(x, pltpu.VMEM)


def split_terms(x):
    high = x.astype(jnp.bfloat16)
    return high, (x - high.astype(jnp.float32)).astype(jnp.bfloat16)


def across(lhs, rhs):
    return lax.dot_general(lhs, rhs, (((1,), (1,)), ((), ())), preferred_element_type=jnp.float32)


def partial_kernel(
    place_ref,
    hidden_hbm,
    gain_ref,
    gate_hbm,
    up_hbm,
    grad_hbm,
    down_hbm,
    send_ref,
    gate,
    up,
    rows_ref,
    kept_gain,
    hidden,
    grad,
    down,
    sems,
):
    moves = [
        pltpu.make_async_copy(source, target, sems.at[i])
        for i, (source, target) in enumerate(
            ((hidden_hbm, hidden), (grad_hbm, grad), (down_hbm, down), (gate_hbm, gate), (up_hbm, up))
        )
    ]
    for move in moves:
        move.start()
    pieces, rows, lanes = send_ref.shape
    units = gate.shape[0]
    ub = units * 2 // pieces

    def pack(part, first):
        for u in range(pieces // 2):
            for half in range(2):
                send_ref[2 * u + half, first : first + ub, :] = part[
                    u * ub : (u + 1) * ub, half * lanes : (half + 1) * lanes
                ].astype(jnp.bfloat16)

    moves[0].wait()
    wide = hidden[...].astype(jnp.float32)
    scaled = (wide * gain_ref[...]).astype(jnp.bfloat16)
    high, low = split_terms(wide * wide)
    ones = jnp.ones((8, hidden.shape[1]), jnp.bfloat16)
    squared = across(ones, high) + across(ones, low)
    high, low = split_terms(squared)
    row = lax.broadcasted_iota(jnp.int32, squared.shape, 0)
    extra = jnp.where(row == 0, high.astype(jnp.float32), jnp.where(row == 1, low.astype(jnp.float32), 0.0))
    for piece in range(pieces):
        half = piece % 2
        send_ref[piece, 3 * ub : rows, :] = extra[:, half * lanes : (half + 1) * lanes].astype(jnp.bfloat16)
    share = rows_ref.shape[1]
    first = pl.multiple_of(place_ref[1], share)
    for l in range(rows_ref.shape[0]):
        rows_ref[l] = hidden[pl.ds(first, share), l * 128 : (l + 1) * 128].astype(jnp.float32)
    kept_gain[...] = gain_ref[...]
    moves[1].wait()
    moves[2].wait()
    pack(across(down[...], grad[...]), 2 * ub)
    moves[3].wait()
    pack(across(gate[...], scaled), 0)
    moves[4].wait()
    pack(across(up[...], scaled), ub)


def partials(place, hidden_in, norm_gain, gate_rows, up_rows, grad_out, down_weight, pieces):
    tokens, width = hidden_in.shape
    units = gate_rows.shape[0]
    share = tokens // 2 // RING
    anywhere = pl.BlockSpec(memory_space=pl.ANY)
    inside = pl.BlockSpec(memory_space=pltpu.VMEM)
    return pl.pallas_call(
        partial_kernel,
        out_shape=(
            pltpu.VMEM((pieces, 3 * (units * 2 // pieces) + 8, tokens // 2), jnp.bfloat16),
            pltpu.VMEM((units, width), jnp.bfloat16),
            pltpu.VMEM((units, width), jnp.bfloat16),
            pltpu.VMEM((width // 128, share, 128), jnp.float32),
            pltpu.VMEM((1, width), jnp.float32),
        ),
        in_specs=[pl.BlockSpec(memory_space=pltpu.SMEM), anywhere, inside, anywhere, anywhere, anywhere, anywhere],
        out_specs=(inside,) * 5,
        scratch_shapes=[
            pltpu.VMEM((tokens, width), jnp.bfloat16),
            pltpu.VMEM((tokens, width), jnp.bfloat16),
            pltpu.VMEM((units, width), jnp.bfloat16),
            pltpu.SemaphoreType.DMA((5,)),
        ],
        name="partials",
    )(place, hidden_in, norm_gain.reshape(1, width), gate_rows, up_rows, grad_out, down_weight)


def piece_kernel(came_ref, out_ref):
    pieces, rows, lanes = came_ref.shape
    ub = (rows - 8) // 3
    got = came_ref[0].astype(jnp.float32)
    for i in range(1, pieces):
        got = got + came_ref[i].astype(jnp.float32)
    square_sum = got[3 * ub : 3 * ub + 1] + got[3 * ub + 1 : 3 * ub + 2]
    inverse = lax.rsqrt(square_sum / D + epsilon)
    gate = inverse * got[:ub]
    up_val = inverse * got[ub : 2 * ub]
    act_grad = got[2 * ub : 3 * ub]
    sigma = jax.nn.sigmoid(gate)
    activation = (gate * sigma * up_val).astype(jnp.bfloat16)
    gate_grad = (inverse * act_grad * up_val * sigma * (1.0 + gate * (1.0 - sigma))).astype(jnp.bfloat16)
    up_grad = (inverse * act_grad * gate * sigma).astype(jnp.bfloat16)
    both = gate_grad.astype(jnp.float32) * gate + up_grad.astype(jnp.float32) * up_val
    pulled = jnp.broadcast_to(inverse * jnp.sum(both, axis=0, keepdims=True) / D, (8, lanes))
    high, low = split_terms(pulled)
    row = lax.broadcasted_iota(jnp.int32, (8, lanes), 0)
    extra = jnp.where(row == 0, high.astype(jnp.float32), jnp.where(row == 1, low.astype(jnp.float32), 0.0))
    extra = extra.astype(jnp.bfloat16)
    for i in range(pieces):
        out_ref[i, :ub, :] = activation
        out_ref[i, ub : 2 * ub, :] = gate_grad
        out_ref[i, 2 * ub : 3 * ub, :] = up_grad
        out_ref[i, 3 * ub :, :] = extra


def row_terms(pulled, used):
    high, low = split_terms(pulled)
    return (high.astype(jnp.float32) + pltpu.roll(low.astype(jnp.float32), used, 0)).astype(jnp.bfloat16)


def term_rows(terms, used):
    row = lax.broadcasted_iota(jnp.int32, (8, 128), 0)
    return jnp.where(row < used, terms + pltpu.roll(terms, 8 - used, 0), 0.0)


def other_kernel(place_ref, part_ref, all_ref, out_ref, pulled_ref):
    tokens, width = part_ref.shape
    half, lanes = tokens // 2, width // 128
    base = pl.multiple_of((1 - place_ref[0]) * half, half)
    for l in range(lanes):
        out_ref[l * half : (l + 1) * half] = part_ref[pl.ds(base, half), l * 128 : (l + 1) * 128].astype(jnp.bfloat16)
    pieces, rows, _ = all_ref.shape
    row = lax.broadcasted_iota(jnp.int32, (8, 128), 0)
    pulled = jnp.zeros((8, 128), jnp.float32)
    for h in range(2):
        got = all_ref[h, rows - 8 :].astype(jnp.float32)
        for i in range(2 + h, pieces, 2):
            got = got + all_ref[i, rows - 8 :].astype(jnp.float32)
        pulled = jnp.where(row == h, got[0:1] + got[1:2], pulled)
    pulled_ref[...] = pulled
    out_ref[lanes * half :] = row_terms(pulled, tokens // 128)


def added_kernel(came_ref, out_ref):
    total = came_ref[0].astype(jnp.float32)
    for k in range(1, came_ref.shape[0]):
        total = total + came_ref[k].astype(jnp.float32)
    rows = total.shape[0] - 8
    out_ref[:rows] = total[:rows]
    out_ref[rows:] = term_rows(total[rows:], 2)


def cuts_kernel(place_ref, part_ref, came_ref, pulled_ref, out_ref):
    ring = out_ref.shape[0]
    tokens, width = part_ref.shape
    half, lanes = tokens // 2, width // 128
    share = half // ring
    base = place_ref[0] * half
    for k in range(ring):
        at = pl.multiple_of(base + k * share, share)
        for l in range(lanes):
            other = came_ref[l * half + k * share : l * half + (k + 1) * share].astype(jnp.float32)
            total = part_ref[pl.ds(at, share), l * 128 : (l + 1) * 128] + other
            out_ref[k, l * share : (l + 1) * share] = total.astype(jnp.bfloat16)
    used = tokens // 128
    pulled = pulled_ref[...] + term_rows(came_ref[half * lanes :].astype(jnp.float32), used)
    extra = row_terms(pulled, used)
    for k in range(ring):
        out_ref[k, lanes * share :] = extra


def owned_kernel(place_ref, all_ref, hidden_ref, gain_ref, out_ref):
    lanes, share, _ = hidden_ref.shape
    total = all_ref[0]
    for i in range(1, all_ref.shape[0]):
        total = total + all_ref[i]
    core, first = place_ref[0], place_ref[1]
    pulled = jnp.where(
        core == 0, total[lanes * share : lanes * share + 1], total[lanes * share + 1 : lanes * share + 2]
    )
    row = lax.broadcasted_iota(jnp.int32, (share, 128), 0)
    lane = lax.broadcasted_iota(jnp.int32, (share, 128), 1)
    here = lane == row + (first - core * 128)
    pulled = jnp.sum(jnp.where(here, jnp.broadcast_to(pulled, (share, 128)), 0.0), axis=1, keepdims=True)
    row = lax.broadcasted_iota(jnp.int32, (8, 128), 0)
    extra = jnp.zeros((8, 128), jnp.float32)
    for l in range(lanes):
        grad = total[l * share : (l + 1) * share]
        wide = hidden_ref[l]
        rows = (gain_ref[:, l * 128 : (l + 1) * 128] * grad - wide * pulled).astype(jnp.bfloat16)
        high, low = split_terms(jnp.broadcast_to(jnp.sum(wide * grad, axis=0, keepdims=True), (8, 128)))
        extra = jnp.where(row == l, high.astype(jnp.float32), extra)
        extra = jnp.where(row == lanes + l, low.astype(jnp.float32), extra)
        for k in range(out_ref.shape[0]):
            out_ref[k, l * share : (l + 1) * share] = rows
    for k in range(out_ref.shape[0]):
        out_ref[k, lanes * share :] = extra.astype(jnp.bfloat16)


def finish_kernel(core_ref, near_ref, pair_ref, rows_ref, gain_ref):
    ring, rows, lane = near_ref.shape
    lanes = rows_ref.shape[1] // lane
    share = (rows - 2 * lanes) // lanes
    first = core_ref[0] == 0
    total = jnp.zeros((lanes, lane), jnp.float32)
    for half in range(2):
        take_near = first if half == 0 else jnp.logical_not(first)
        for k in range(ring):
            got = jnp.where(take_near, near_ref[k].astype(jnp.float32), pair_ref[k].astype(jnp.float32))
            at = (half * ring + k) * share
            for l in range(lanes):
                rows_ref[at : at + share, l * lane : (l + 1) * lane] = got[l * share : (l + 1) * share].astype(jnp.bfloat16)
            total = total + (got[lanes * share : lanes * share + lanes] + got[lanes * share + lanes :])
    gain_ref[...] = total


def body(hidden_in, norm_gain, grad_out, gate_weight, up_weight, down_weight):
    f32, bf16 = jnp.float32, jnp.bfloat16
    tokens, width = hidden_in.shape
    units = gate_weight.shape[1]
    mp, ffn = lax.axis_size("mp"), lax.axis_size("ffn")
    ublocks, thalf = mp // 2, tokens // 2
    ub = units // ublocks
    levels = ffn // 2 // RING
    me = lax.axis_index("ffn").astype(jnp.uint32)
    core, z = me % 2, me // 2
    first = core * thalf + z % RING * (thalf // RING)
    hidden_in, core, first = lax.optimization_barrier((hidden_in, core, first))

    place = jnp.stack([core, first]).astype(jnp.int32)
    send, gate_rows, up_rows, rows_hidden, kept_gain = partials(
        place, hidden_in, norm_gain, gate_weight.T, up_weight.T, grad_out, down_weight, mp
    )
    scaled = (hidden_in.astype(f32) * norm_gain).astype(bf16)
    came = lax.all_to_all(send, "mp", 0, 0, tiled=True)
    piece = pl.pallas_call(
        piece_kernel, out_shape=pltpu.VMEM(came.shape, bf16), name="piece"
    )(in_vmem(came))
    everything_flat = lax.all_to_all(piece, "mp", 0, 0, tiled=True)
    everything = everything_flat.reshape(ublocks, 2, 3 * ub + 8, thalf)

    def joined(k):
        part = everything[:, :, k * ub : (k + 1) * ub]
        return part.transpose(0, 2, 1, 3).reshape(units, tokens)

    act_t, gate_grad_t, up_grad_t = joined(0), joined(1), joined(2)
    input_part = lax.dot_general(
        gate_grad_t, gate_rows, (((0,), (0,)), ((), ())), preferred_element_type=f32
    ) + lax.dot_general(up_grad_t, up_rows, (((0,), (0,)), ((), ())), preferred_element_type=f32)

    lanes = width // 128
    smem, inside = pl.BlockSpec(memory_space=pltpu.SMEM), pl.BlockSpec(memory_space=pltpu.VMEM)
    input_part = in_vmem(input_part)
    packed, pulled = pl.pallas_call(
        other_kernel,
        out_shape=(pltpu.VMEM((thalf * lanes + 8, 128), bf16), pltpu.VMEM((8, 128), f32)),
        in_specs=[smem, inside, inside],
        out_specs=(inside, inside),
        name="other",
    )(place, input_part, in_vmem(everything_flat))
    pair = [(i, i ^ 1) for i in range(ffn)]
    came = lax.ppermute(packed, "ffn", pair)
    share = thalf // RING
    near = [[(g * RING + j) * 2 + c for j in range(RING)] for g in range(levels) for c in range(2)]
    cuts = pl.pallas_call(
        cuts_kernel,
        out_shape=pltpu.VMEM((RING, share * lanes + 8, 128), bf16),
        in_specs=[smem, inside, inside, inside],
        out_specs=inside,
        name="cuts",
    )(place, input_part, in_vmem(came), in_vmem(pulled))
    came = lax.all_to_all(cuts, "ffn", 0, 0, tiled=True, axis_index_groups=near)

    packed = pl.pallas_call(
        added_kernel, out_shape=pltpu.VMEM(came.shape[1:], f32), name="added"
    )(in_vmem(came))
    owners = [[(k * RING + j) * 2 + c for k in range(levels)] for j in range(RING) for c in range(2)]
    everyone = lax.all_gather(packed, "ffn", axis_index_groups=owners)
    piece = pl.pallas_call(
        owned_kernel,
        out_shape=jax.ShapeDtypeStruct((RING, share * lanes + 8, 128), bf16),
        in_specs=[smem, inside, inside, inside],
        out_specs=inside,
        name="owned",
    )(place, in_vmem(everyone), in_vmem(rows_hidden), in_vmem(kept_gain))

    near_rows = lax.all_to_all(piece, "ffn", 0, 0, tiled=True, axis_index_groups=near)
    pair_rows = lax.ppermute(near_rows, "ffn", pair)
    grad_hidden, grad_gain = pl.pallas_call(
        finish_kernel,
        out_shape=(jax.ShapeDtypeStruct((tokens, width), bf16), jax.ShapeDtypeStruct((lanes, 128), f32)),
        in_specs=[smem, inside, inside],
        out_specs=(inside, inside),
        name="finish",
    )(place, in_vmem(near_rows), in_vmem(pair_rows))
    grad_gain = grad_gain.reshape(width)

    def weight_grad(lhs, rhs, dims):
        return lax.dot_general(lhs, rhs, (dims, ((), ())), preferred_element_type=f32).astype(bf16)

    grad_down = weight_grad(act_t, grad_out, ((1,), (0,)))
    grad_gate = weight_grad(scaled, gate_grad_t, ((0,), (1,)))
    grad_up = weight_grad(scaled, up_grad_t, ((0,), (1,)))
    return (grad_hidden, grad_gain, grad_gate, grad_up, grad_down)


def solution(mesh):
    placed = (P(None, "mp"), P("mp"), P(None, "mp"), P("mp", "ffn"), P("mp", "ffn"), P("ffn", "mp"))
    return jax.shard_map(
        body,
        mesh=mesh,
        in_specs=placed,
        out_specs=(P(None, "mp"), P("mp"), P("mp", "ffn"), P("mp", "ffn"), P("ffn", "mp")),
        check_vma=False,
    )
```

```python
import jax
import jax.numpy as jnp
from jax import lax
from jax.experimental import pallas as pl
from jax.experimental.pallas import tpu as pltpu
from jax.sharding import PartitionSpec as P

D = 8192
epsilon = 1e-05
RING = 8


def in_vmem(x):
    return pltpu.with_memory_space_constraint(x, pltpu.VMEM)


def place(tokens, share):
    me = lax.axis_index("ffn")
    core = lax.rem(me, 2)
    return core, core * (tokens // 2) + lax.rem(lax.div(me, 2), RING) * share


def split_terms(x):
    high = x.astype(jnp.bfloat16)
    return high, (x - high.astype(jnp.float32)).astype(jnp.bfloat16)


def across(lhs, rhs):
    return lax.dot_general(lhs, rhs, (((1,), (1,)), ((), ())), preferred_element_type=jnp.float32)


def partial_kernel(
    hidden_hbm,
    gain_ref,
    gate_hbm,
    up_hbm,
    grad_hbm,
    down_hbm,
    send_ref,
    gate,
    up,
    rows_ref,
    kept_gain,
    hidden,
    grad,
    down,
    sems,
):
    moves = [
        pltpu.make_async_copy(source, target, sems.at[i])
        for i, (source, target) in enumerate(
            ((hidden_hbm, hidden), (grad_hbm, grad), (down_hbm, down), (gate_hbm, gate), (up_hbm, up))
        )
    ]
    for move in moves:
        move.start()
    pieces, rows, lanes = send_ref.shape
    units = gate.shape[0]
    ub = units * 2 // pieces

    def pack(part, first):
        for u in range(pieces // 2):
            for half in range(2):
                send_ref[2 * u + half, first : first + ub, :] = part[
                    u * ub : (u + 1) * ub, half * lanes : (half + 1) * lanes
                ].astype(jnp.bfloat16)

    moves[0].wait()
    wide = hidden[...].astype(jnp.float32)
    scaled = (wide * gain_ref[...]).astype(jnp.bfloat16)
    high, low = split_terms(wide * wide)
    ones = jnp.ones((8, hidden.shape[1]), jnp.bfloat16)
    squared = across(ones, high) + across(ones, low)
    high, low = split_terms(squared)
    row = lax.broadcasted_iota(jnp.int32, squared.shape, 0)
    extra = jnp.where(row == 0, high.astype(jnp.float32), jnp.where(row == 1, low.astype(jnp.float32), 0.0))
    for piece in range(pieces):
        half = piece % 2
        send_ref[piece, 3 * ub : rows, :] = extra[:, half * lanes : (half + 1) * lanes].astype(jnp.bfloat16)
    share = rows_ref.shape[1]
    first = pl.multiple_of(place(hidden.shape[0], share)[1], share)
    for l in range(rows_ref.shape[0]):
        rows_ref[l] = hidden[pl.ds(first, share), l * 128 : (l + 1) * 128].astype(jnp.float32)
    kept_gain[...] = gain_ref[...]
    moves[1].wait()
    moves[2].wait()
    pack(across(down[...], grad[...]), 2 * ub)
    moves[3].wait()
    pack(across(gate[...], scaled), 0)
    moves[4].wait()
    pack(across(up[...], scaled), ub)


def partials(hidden_in, norm_gain, gate_rows, up_rows, grad_out, down_weight, pieces):
    tokens, width = hidden_in.shape
    units = gate_rows.shape[0]
    share = tokens // 2 // RING
    anywhere = pl.BlockSpec(memory_space=pl.ANY)
    inside = pl.BlockSpec(memory_space=pltpu.VMEM)
    return pl.pallas_call(
        partial_kernel,
        out_shape=(
            pltpu.VMEM((pieces, 3 * (units * 2 // pieces) + 8, tokens // 2), jnp.bfloat16),
            pltpu.VMEM((units, width), jnp.bfloat16),
            pltpu.VMEM((units, width), jnp.bfloat16),
            pltpu.VMEM((width // 128, share, 128), jnp.float32),
            pltpu.VMEM((1, width), jnp.float32),
        ),
        in_specs=[anywhere, inside, anywhere, anywhere, anywhere, anywhere],
        out_specs=(inside,) * 5,
        scratch_shapes=[
            pltpu.VMEM((tokens, width), jnp.bfloat16),
            pltpu.VMEM((tokens, width), jnp.bfloat16),
            pltpu.VMEM((units, width), jnp.bfloat16),
            pltpu.SemaphoreType.DMA((5,)),
        ],
        name="partials",
    )(hidden_in, norm_gain.reshape(1, width), gate_rows, up_rows, grad_out, down_weight)


def piece_kernel(came_ref, out_ref):
    pieces, rows, lanes = came_ref.shape
    ub = (rows - 8) // 3
    got = came_ref[0].astype(jnp.float32)
    for i in range(1, pieces):
        got = got + came_ref[i].astype(jnp.float32)
    square_sum = got[3 * ub : 3 * ub + 1] + got[3 * ub + 1 : 3 * ub + 2]
    inverse = lax.rsqrt(square_sum / D + epsilon)
    gate = inverse * got[:ub]
    up_val = inverse * got[ub : 2 * ub]
    act_grad = got[2 * ub : 3 * ub]
    sigma = jax.nn.sigmoid(gate)
    activation = (gate * sigma * up_val).astype(jnp.bfloat16)
    gate_grad = (inverse * act_grad * up_val * sigma * (1.0 + gate * (1.0 - sigma))).astype(jnp.bfloat16)
    up_grad = (inverse * act_grad * gate * sigma).astype(jnp.bfloat16)
    both = gate_grad.astype(jnp.float32) * gate + up_grad.astype(jnp.float32) * up_val
    pulled = jnp.broadcast_to(inverse * jnp.sum(both, axis=0, keepdims=True) / D, (8, lanes))
    high, low = split_terms(pulled)
    row = lax.broadcasted_iota(jnp.int32, (8, lanes), 0)
    extra = jnp.where(row == 0, high.astype(jnp.float32), jnp.where(row == 1, low.astype(jnp.float32), 0.0))
    extra = extra.astype(jnp.bfloat16)
    for i in range(pieces):
        out_ref[i, :ub, :] = activation
        out_ref[i, ub : 2 * ub, :] = gate_grad
        out_ref[i, 2 * ub : 3 * ub, :] = up_grad
        out_ref[i, 3 * ub :, :] = extra


def row_terms(pulled, used):
    high, low = split_terms(pulled)
    return (high.astype(jnp.float32) + pltpu.roll(low.astype(jnp.float32), used, 0)).astype(jnp.bfloat16)


def term_rows(terms, used):
    row = lax.broadcasted_iota(jnp.int32, (8, 128), 0)
    return jnp.where(row < used, terms + pltpu.roll(terms, 8 - used, 0), 0.0)


def other_kernel(gate_ref, up_ref, all_ref, out_ref, part_ref, pulled_ref, gate_grad, up_grad):
    tokens, width = part_ref.shape
    half, lanes = tokens // 2, width // 128
    pieces, rows, _ = all_ref.shape
    ub = (rows - 8) // 3
    for i in range(pieces):
        u, h = i // 2, i % 2
        gate_grad[u * ub : (u + 1) * ub, h * half : (h + 1) * half] = all_ref[i, ub : 2 * ub]
        up_grad[u * ub : (u + 1) * ub, h * half : (h + 1) * half] = all_ref[i, 2 * ub : 3 * ub]

    def down_first(lhs, rhs):
        return lax.dot_general(lhs, rhs, (((0,), (0,)), ((), ())), preferred_element_type=jnp.float32)

    part_ref[...] = down_first(gate_grad[...], gate_ref[...]) + down_first(up_grad[...], up_ref[...])
    base = pl.multiple_of((1 - place(tokens, 1)[0]) * half, half)
    for l in range(lanes):
        out_ref[l * half : (l + 1) * half] = part_ref[pl.ds(base, half), l * 128 : (l + 1) * 128].astype(jnp.bfloat16)
    row = lax.broadcasted_iota(jnp.int32, (8, 128), 0)
    pulled = jnp.zeros((8, 128), jnp.float32)
    for h in range(2):
        got = all_ref[h, rows - 8 :].astype(jnp.float32)
        for i in range(2 + h, pieces, 2):
            got = got + all_ref[i, rows - 8 :].astype(jnp.float32)
        pulled = jnp.where(row == h, got[0:1] + got[1:2], pulled)
    pulled_ref[...] = pulled
    out_ref[lanes * half :] = row_terms(pulled, tokens // 128)


def added_kernel(came_ref, out_ref):
    total = came_ref[0].astype(jnp.float32)
    for k in range(1, came_ref.shape[0]):
        total = total + came_ref[k].astype(jnp.float32)
    rows = total.shape[0] - 8
    out_ref[:rows] = total[:rows]
    out_ref[rows:] = term_rows(total[rows:], 2)


def cuts_kernel(part_ref, came_ref, pulled_ref, out_ref):
    ring = out_ref.shape[0]
    tokens, width = part_ref.shape
    half, lanes = tokens // 2, width // 128
    share = half // ring
    base = place(tokens, share)[0] * half
    for k in range(ring):
        at = pl.multiple_of(base + k * share, share)
        for l in range(lanes):
            other = came_ref[l * half + k * share : l * half + (k + 1) * share].astype(jnp.float32)
            total = part_ref[pl.ds(at, share), l * 128 : (l + 1) * 128] + other
            out_ref[k, l * share : (l + 1) * share] = total.astype(jnp.bfloat16)
    used = tokens // 128
    pulled = pulled_ref[...] + term_rows(came_ref[half * lanes :].astype(jnp.float32), used)
    extra = row_terms(pulled, used)
    for k in range(ring):
        out_ref[k, lanes * share :] = extra


def owned_kernel(all_ref, hidden_ref, gain_ref, out_ref):
    lanes, share, _ = hidden_ref.shape
    total = all_ref[0]
    for i in range(1, all_ref.shape[0]):
        total = total + all_ref[i]
    core, first = place(share * RING * 2, share)
    pulled = jnp.where(
        core == 0, total[lanes * share : lanes * share + 1], total[lanes * share + 1 : lanes * share + 2]
    )
    row = lax.broadcasted_iota(jnp.int32, (share, 128), 0)
    lane = lax.broadcasted_iota(jnp.int32, (share, 128), 1)
    here = lane == row + (first - core * 128)
    pulled = jnp.sum(jnp.where(here, jnp.broadcast_to(pulled, (share, 128)), 0.0), axis=1, keepdims=True)
    row = lax.broadcasted_iota(jnp.int32, (8, 128), 0)
    extra = jnp.zeros((8, 128), jnp.float32)
    for l in range(lanes):
        grad = total[l * share : (l + 1) * share]
        wide = hidden_ref[l]
        rows = (gain_ref[:, l * 128 : (l + 1) * 128] * grad - wide * pulled).astype(jnp.bfloat16)
        high, low = split_terms(jnp.broadcast_to(jnp.sum(wide * grad, axis=0, keepdims=True), (8, 128)))
        extra = jnp.where(row == l, high.astype(jnp.float32), extra)
        extra = jnp.where(row == lanes + l, low.astype(jnp.float32), extra)
        for k in range(out_ref.shape[0]):
            out_ref[k, l * share : (l + 1) * share] = rows
    for k in range(out_ref.shape[0]):
        out_ref[k, lanes * share :] = extra.astype(jnp.bfloat16)


def finish_kernel(near_ref, pair_ref, rows_ref, gain_ref):
    ring, rows, lane = near_ref.shape
    lanes = rows_ref.shape[1] // lane
    share = (rows - 2 * lanes) // lanes
    first = place(rows_ref.shape[0], share)[0] == 0
    total = jnp.zeros((lanes, lane), jnp.float32)
    for half in range(2):
        take_near = first if half == 0 else jnp.logical_not(first)
        for k in range(ring):
            got = jnp.where(take_near, near_ref[k].astype(jnp.float32), pair_ref[k].astype(jnp.float32))
            at = (half * ring + k) * share
            for l in range(lanes):
                rows_ref[at : at + share, l * lane : (l + 1) * lane] = got[l * share : (l + 1) * share].astype(jnp.bfloat16)
            total = total + (got[lanes * share : lanes * share + lanes] + got[lanes * share + lanes :])
    gain_ref[...] = total


def body(hidden_in, norm_gain, grad_out, gate_weight, up_weight, down_weight):
    f32, bf16 = jnp.float32, jnp.bfloat16
    tokens, width = hidden_in.shape
    units = gate_weight.shape[1]
    mp, ffn = lax.axis_size("mp"), lax.axis_size("ffn")
    ublocks, thalf = mp // 2, tokens // 2
    ub = units // ublocks
    levels = ffn // 2 // RING
    send, gate_rows, up_rows, rows_hidden, kept_gain = partials(
        hidden_in, norm_gain, gate_weight.T, up_weight.T, grad_out, down_weight, mp
    )
    scaled = (hidden_in.astype(f32) * norm_gain).astype(bf16)
    came = lax.all_to_all(send, "mp", 0, 0, tiled=True)
    piece = pl.pallas_call(
        piece_kernel, out_shape=pltpu.VMEM(came.shape, bf16), name="piece"
    )(in_vmem(came))
    everything_flat = lax.all_to_all(piece, "mp", 0, 0, tiled=True)
    everything = everything_flat.reshape(ublocks, 2, 3 * ub + 8, thalf)

    def joined(k):
        part = everything[:, :, k * ub : (k + 1) * ub]
        return part.transpose(0, 2, 1, 3).reshape(units, tokens)

    act_t, gate_grad_t, up_grad_t = joined(0), joined(1), joined(2)
    lanes = width // 128
    inside = pl.BlockSpec(memory_space=pltpu.VMEM)
    packed, input_part, pulled = pl.pallas_call(
        other_kernel,
        out_shape=(
            pltpu.VMEM((thalf * lanes + 8, 128), bf16),
            pltpu.VMEM((tokens, width), f32),
            pltpu.VMEM((8, 128), f32),
        ),
        scratch_shapes=[pltpu.VMEM((units, tokens), bf16), pltpu.VMEM((units, tokens), bf16)],
        name="other",
    )(in_vmem(gate_rows), in_vmem(up_rows), in_vmem(everything_flat))
    pair = [(i, i ^ 1) for i in range(ffn)]
    came = lax.ppermute(packed, "ffn", pair)
    share = thalf // RING
    near = [[(g * RING + j) * 2 + c for j in range(RING)] for g in range(levels) for c in range(2)]
    cuts = pl.pallas_call(
        cuts_kernel,
        out_shape=pltpu.VMEM((RING, share * lanes + 8, 128), bf16),
        in_specs=[inside, inside, inside],
        out_specs=inside,
        name="cuts",
    )(in_vmem(input_part), in_vmem(came), in_vmem(pulled))
    came = lax.all_to_all(cuts, "ffn", 0, 0, tiled=True, axis_index_groups=near)

    packed = pl.pallas_call(
        added_kernel, out_shape=pltpu.VMEM(came.shape[1:], f32), name="added"
    )(in_vmem(came))
    owners = [[(k * RING + j) * 2 + c for k in range(levels)] for j in range(RING) for c in range(2)]
    everyone = lax.all_gather(packed, "ffn", axis_index_groups=owners)
    piece = pl.pallas_call(
        owned_kernel,
        out_shape=jax.ShapeDtypeStruct((RING, share * lanes + 8, 128), bf16),
        in_specs=[inside, inside, inside],
        out_specs=inside,
        name="owned",
    )(in_vmem(everyone), in_vmem(rows_hidden), in_vmem(kept_gain))

    near_rows = lax.all_to_all(piece, "ffn", 0, 0, tiled=True, axis_index_groups=near)
    pair_rows = lax.ppermute(near_rows, "ffn", pair)
    grad_hidden, grad_gain = pl.pallas_call(
        finish_kernel,
        out_shape=(jax.ShapeDtypeStruct((tokens, width), bf16), jax.ShapeDtypeStruct((lanes, 128), f32)),
        in_specs=[inside, inside],
        out_specs=(inside, inside),
        name="finish",
    )(in_vmem(near_rows), in_vmem(pair_rows))
    grad_gain = grad_gain.reshape(width)

    def weight_grad(lhs, rhs, dims):
        return lax.dot_general(lhs, rhs, (dims, ((), ())), preferred_element_type=f32).astype(bf16)

    grad_down = weight_grad(act_t, grad_out, ((1,), (0,)))
    grad_gate = weight_grad(scaled, gate_grad_t, ((0,), (1,)))
    grad_up = weight_grad(scaled, up_grad_t, ((0,), (1,)))
    return (grad_hidden, grad_gain, grad_gate, grad_up, grad_down)


def solution(mesh):
    placed = (P(None, "mp"), P("mp"), P(None, "mp"), P("mp", "ffn"), P("mp", "ffn"), P("ffn", "mp"))
    return jax.shard_map(
        body,
        mesh=mesh,
        in_specs=placed,
        out_specs=(P(None, "mp"), P("mp"), P("mp", "ffn"), P("mp", "ffn"), P("ffn", "mp")),
        check_vma=False,
    )
```

```python
import jax
import jax.numpy as jnp
from jax import lax
from jax.experimental import pallas as pl
from jax.experimental.pallas import tpu as pltpu
from jax.sharding import PartitionSpec as P

D = 8192
epsilon = 1e-05
RING = 4


def in_vmem(x):
    return pltpu.with_memory_space_constraint(x, pltpu.VMEM)


def place(tokens, share):
    me = lax.axis_index("ffn")
    core = lax.rem(me, 2)
    return core, core * (tokens // 2) + lax.rem(lax.div(me, 2), RING) * share


def split_terms(x):
    high = x.astype(jnp.bfloat16)
    return high, (x - high.astype(jnp.float32)).astype(jnp.bfloat16)


def across(lhs, rhs):
    return lax.dot_general(lhs, rhs, (((1,), (1,)), ((), ())), preferred_element_type=jnp.float32)


def partial_kernel(
    hidden_hbm,
    gain_ref,
    gate_hbm,
    up_hbm,
    grad_hbm,
    down_hbm,
    send_ref,
    gate,
    up,
    rows_ref,
    kept_gain,
    hidden,
    grad,
    down,
    sems,
):
    moves = [
        pltpu.make_async_copy(source, target, sems.at[i])
        for i, (source, target) in enumerate(
            ((hidden_hbm, hidden), (grad_hbm, grad), (down_hbm, down), (gate_hbm, gate), (up_hbm, up))
        )
    ]
    for move in moves:
        move.start()
    pieces, rows, lanes = send_ref.shape
    units = gate.shape[0]
    ub = units * 2 // pieces

    def pack(part, first):
        for u in range(pieces // 2):
            for half in range(2):
                send_ref[2 * u + half, first : first + ub, :] = part[
                    u * ub : (u + 1) * ub, half * lanes : (half + 1) * lanes
                ].astype(jnp.bfloat16)

    moves[0].wait()
    wide = hidden[...].astype(jnp.float32)
    scaled = (wide * gain_ref[...]).astype(jnp.bfloat16)
    high, low = split_terms(wide * wide)
    ones = jnp.ones((8, hidden.shape[1]), jnp.bfloat16)
    squared = across(ones, high) + across(ones, low)
    high, low = split_terms(squared)
    row = lax.broadcasted_iota(jnp.int32, squared.shape, 0)
    extra = jnp.where(row == 0, high.astype(jnp.float32), jnp.where(row == 1, low.astype(jnp.float32), 0.0))
    for piece in range(pieces):
        half = piece % 2
        send_ref[piece, 3 * ub : rows, :] = extra[:, half * lanes : (half + 1) * lanes].astype(jnp.bfloat16)
    share = rows_ref.shape[1]
    first = pl.multiple_of(place(hidden.shape[0], share)[1], share)
    for l in range(rows_ref.shape[0]):
        rows_ref[l] = hidden[pl.ds(first, share), l * 128 : (l + 1) * 128].astype(jnp.float32)
    kept_gain[...] = gain_ref[...]
    moves[1].wait()
    moves[2].wait()
    pack(across(down[...], grad[...]), 2 * ub)
    moves[3].wait()
    pack(across(gate[...], scaled), 0)
    moves[4].wait()
    pack(across(up[...], scaled), ub)


def partials(hidden_in, norm_gain, gate_rows, up_rows, grad_out, down_weight, pieces):
    tokens, width = hidden_in.shape
    units = gate_rows.shape[0]
    share = tokens // 2 // RING
    anywhere = pl.BlockSpec(memory_space=pl.ANY)
    inside = pl.BlockSpec(memory_space=pltpu.VMEM)
    return pl.pallas_call(
        partial_kernel,
        out_shape=(
            pltpu.VMEM((pieces, 3 * (units * 2 // pieces) + 8, tokens // 2), jnp.bfloat16),
            pltpu.VMEM((units, width), jnp.bfloat16),
            pltpu.VMEM((units, width), jnp.bfloat16),
            pltpu.VMEM((width // 128, share, 128), jnp.float32),
            pltpu.VMEM((1, width), jnp.float32),
        ),
        in_specs=[anywhere, inside, anywhere, anywhere, anywhere, anywhere],
        out_specs=(inside,) * 5,
        scratch_shapes=[
            pltpu.VMEM((tokens, width), jnp.bfloat16),
            pltpu.VMEM((tokens, width), jnp.bfloat16),
            pltpu.VMEM((units, width), jnp.bfloat16),
            pltpu.SemaphoreType.DMA((5,)),
        ],
        name="partials",
    )(hidden_in, norm_gain.reshape(1, width), gate_rows, up_rows, grad_out, down_weight)


def piece_kernel(came_ref, out_ref):
    pieces, rows, lanes = came_ref.shape
    ub = (rows - 8) // 3
    got = came_ref[0].astype(jnp.float32)
    for i in range(1, pieces):
        got = got + came_ref[i].astype(jnp.float32)
    square_sum = got[3 * ub : 3 * ub + 1] + got[3 * ub + 1 : 3 * ub + 2]
    inverse = lax.rsqrt(square_sum / D + epsilon)
    gate = inverse * got[:ub]
    up_val = inverse * got[ub : 2 * ub]
    act_grad = got[2 * ub : 3 * ub]
    sigma = jax.nn.sigmoid(gate)
    activation = (gate * sigma * up_val).astype(jnp.bfloat16)
    gate_grad = (inverse * act_grad * up_val * sigma * (1.0 + gate * (1.0 - sigma))).astype(jnp.bfloat16)
    up_grad = (inverse * act_grad * gate * sigma).astype(jnp.bfloat16)
    both = gate_grad.astype(jnp.float32) * gate + up_grad.astype(jnp.float32) * up_val
    pulled = jnp.broadcast_to(inverse * jnp.sum(both, axis=0, keepdims=True) / D, (8, lanes))
    high, low = split_terms(pulled)
    row = lax.broadcasted_iota(jnp.int32, (8, lanes), 0)
    extra = jnp.where(row == 0, high.astype(jnp.float32), jnp.where(row == 1, low.astype(jnp.float32), 0.0))
    extra = extra.astype(jnp.bfloat16)
    for i in range(pieces):
        out_ref[i, :ub, :] = activation
        out_ref[i, ub : 2 * ub, :] = gate_grad
        out_ref[i, 2 * ub : 3 * ub, :] = up_grad
        out_ref[i, 3 * ub :, :] = extra


def row_terms(pulled, used):
    high, low = split_terms(pulled)
    return (high.astype(jnp.float32) + pltpu.roll(low.astype(jnp.float32), used, 0)).astype(jnp.bfloat16)


def term_rows(terms, used):
    row = lax.broadcasted_iota(jnp.int32, (8, 128), 0)
    return jnp.where(row < used, terms + pltpu.roll(terms, 8 - used, 0), 0.0)


def other_kernel(gate_ref, up_ref, all_ref, out_ref, part_ref, pulled_ref, gate_grad, up_grad):
    tokens, width = part_ref.shape
    half, lanes = tokens // 2, width // 128
    pieces, rows, _ = all_ref.shape
    ub = (rows - 8) // 3
    for i in range(pieces):
        u, h = i // 2, i % 2
        gate_grad[u * ub : (u + 1) * ub, h * half : (h + 1) * half] = all_ref[i, ub : 2 * ub]
        up_grad[u * ub : (u + 1) * ub, h * half : (h + 1) * half] = all_ref[i, 2 * ub : 3 * ub]

    def down_first(lhs, rhs):
        return lax.dot_general(lhs, rhs, (((0,), (0,)), ((), ())), preferred_element_type=jnp.float32)

    part_ref[...] = down_first(gate_grad[...], gate_ref[...]) + down_first(up_grad[...], up_ref[...])
    base = pl.multiple_of((1 - place(tokens, 1)[0]) * half, half)
    for l in range(lanes):
        out_ref[l * half : (l + 1) * half] = part_ref[pl.ds(base, half), l * 128 : (l + 1) * 128].astype(jnp.bfloat16)
    row = lax.broadcasted_iota(jnp.int32, (8, 128), 0)
    pulled = jnp.zeros((8, 128), jnp.float32)
    for h in range(2):
        got = all_ref[h, rows - 8 :].astype(jnp.float32)
        for i in range(2 + h, pieces, 2):
            got = got + all_ref[i, rows - 8 :].astype(jnp.float32)
        pulled = jnp.where(row == h, got[0:1] + got[1:2], pulled)
    pulled_ref[...] = pulled
    out_ref[lanes * half :] = row_terms(pulled, tokens // 128)


def added_kernel(came_ref, out_ref):
    total = came_ref[0].astype(jnp.float32)
    for k in range(1, came_ref.shape[0]):
        total = total + came_ref[k].astype(jnp.float32)
    rows = total.shape[0] - 8
    out_ref[:rows] = total[:rows].astype(jnp.bfloat16)
    out_ref[rows:] = row_terms(term_rows(total[rows:], 2), 2)


def cuts_kernel(part_ref, came_ref, pulled_ref, out_ref):
    ring = out_ref.shape[0]
    tokens, width = part_ref.shape
    half, lanes = tokens // 2, width // 128
    share = half // ring
    base = place(tokens, share)[0] * half
    for k in range(ring):
        at = pl.multiple_of(base + k * share, share)
        for l in range(lanes):
            other = came_ref[l * half + k * share : l * half + (k + 1) * share].astype(jnp.float32)
            total = part_ref[pl.ds(at, share), l * 128 : (l + 1) * 128] + other
            out_ref[k, l * share : (l + 1) * share] = total.astype(jnp.bfloat16)
    used = tokens // 128
    pulled = pulled_ref[...] + term_rows(came_ref[half * lanes :].astype(jnp.float32), used)
    extra = row_terms(pulled, used)
    for k in range(ring):
        out_ref[k, lanes * share :] = extra


def owned_kernel(all_ref, hidden_ref, gain_ref, out_ref):
    lanes, share, _ = hidden_ref.shape
    total = all_ref[0].astype(jnp.float32)
    for i in range(1, all_ref.shape[0]):
        total = total + all_ref[i].astype(jnp.float32)
    core, first = place(share * RING * 2, share)
    pulled = term_rows(total[lanes * share :], 2)
    pulled = jnp.where(core == 0, pulled[0:1], pulled[1:2])
    row = lax.broadcasted_iota(jnp.int32, (share, 128), 0)
    lane = lax.broadcasted_iota(jnp.int32, (share, 128), 1)
    here = lane == row + (first - core * 128)
    pulled = jnp.sum(jnp.where(here, jnp.broadcast_to(pulled, (share, 128)), 0.0), axis=1, keepdims=True)
    row = lax.broadcasted_iota(jnp.int32, (8, 128), 0)
    extra = jnp.zeros((8, 128), jnp.float32)
    for l in range(lanes):
        grad = total[l * share : (l + 1) * share]
        wide = hidden_ref[l]
        rows = (gain_ref[:, l * 128 : (l + 1) * 128] * grad - wide * pulled).astype(jnp.bfloat16)
        high, low = split_terms(jnp.broadcast_to(jnp.sum(wide * grad, axis=0, keepdims=True), (8, 128)))
        extra = jnp.where(row == l, high.astype(jnp.float32), extra)
        extra = jnp.where(row == lanes + l, low.astype(jnp.float32), extra)
        for k in range(out_ref.shape[0]):
            out_ref[k, l * share : (l + 1) * share] = rows
    for k in range(out_ref.shape[0]):
        out_ref[k, lanes * share :] = extra.astype(jnp.bfloat16)


def finish_kernel(near_ref, pair_ref, rows_ref, gain_ref):
    ring, rows, lane = near_ref.shape
    lanes = rows_ref.shape[1] // lane
    share = (rows - 2 * lanes) // lanes
    first = place(rows_ref.shape[0], share)[0] == 0
    total = jnp.zeros((lanes, lane), jnp.float32)
    for half in range(2):
        take_near = first if half == 0 else jnp.logical_not(first)
        for k in range(ring):
            got = jnp.where(take_near, near_ref[k].astype(jnp.float32), pair_ref[k].astype(jnp.float32))
            at = (half * ring + k) * share
            for l in range(lanes):
                rows_ref[at : at + share, l * lane : (l + 1) * lane] = got[l * share : (l + 1) * share].astype(jnp.bfloat16)
            total = total + (got[lanes * share : lanes * share + lanes] + got[lanes * share + lanes :])
    gain_ref[...] = total


def body(hidden_in, norm_gain, grad_out, gate_weight, up_weight, down_weight):
    f32, bf16 = jnp.float32, jnp.bfloat16
    tokens, width = hidden_in.shape
    units = gate_weight.shape[1]
    mp, ffn = lax.axis_size("mp"), lax.axis_size("ffn")
    ublocks, thalf = mp // 2, tokens // 2
    ub = units // ublocks
    levels = ffn // 2 // RING
    send, gate_rows, up_rows, rows_hidden, kept_gain = partials(
        hidden_in, norm_gain, gate_weight.T, up_weight.T, grad_out, down_weight, mp
    )
    scaled = (hidden_in.astype(f32) * norm_gain).astype(bf16)
    came = lax.all_to_all(send, "mp", 0, 0, tiled=True)
    piece = pl.pallas_call(
        piece_kernel, out_shape=pltpu.VMEM(came.shape, bf16), name="piece"
    )(in_vmem(came))
    everything_flat = lax.all_to_all(piece, "mp", 0, 0, tiled=True)
    everything = everything_flat.reshape(ublocks, 2, 3 * ub + 8, thalf)

    def joined(k):
        part = everything[:, :, k * ub : (k + 1) * ub]
        return part.transpose(0, 2, 1, 3).reshape(units, tokens)

    act_t, gate_grad_t, up_grad_t = joined(0), joined(1), joined(2)
    lanes = width // 128
    inside = pl.BlockSpec(memory_space=pltpu.VMEM)
    packed, input_part, pulled = pl.pallas_call(
        other_kernel,
        out_shape=(
            pltpu.VMEM((thalf * lanes + 8, 128), bf16),
            pltpu.VMEM((tokens, width), f32),
            pltpu.VMEM((8, 128), f32),
        ),
        scratch_shapes=[pltpu.VMEM((units, tokens), bf16), pltpu.VMEM((units, tokens), bf16)],
        name="other",
    )(in_vmem(gate_rows), in_vmem(up_rows), in_vmem(everything_flat))
    pair = [(i, i ^ 1) for i in range(ffn)]
    came = lax.ppermute(packed, "ffn", pair)
    share = thalf // RING
    near = [[(g * RING + j) * 2 + c for j in range(RING)] for g in range(levels) for c in range(2)]
    cuts = pl.pallas_call(
        cuts_kernel,
        out_shape=pltpu.VMEM((RING, share * lanes + 8, 128), bf16),
        in_specs=[inside, inside, inside],
        out_specs=inside,
        name="cuts",
    )(in_vmem(input_part), in_vmem(came), in_vmem(pulled))
    came = lax.all_to_all(cuts, "ffn", 0, 0, tiled=True, axis_index_groups=near)

    packed = pl.pallas_call(
        added_kernel, out_shape=pltpu.VMEM(came.shape[1:], bf16), name="added"
    )(in_vmem(came))
    owners = [[(k * RING + j) * 2 + c for k in range(levels)] for j in range(RING) for c in range(2)]
    everyone = lax.all_gather(packed, "ffn", axis_index_groups=owners)
    piece = pl.pallas_call(
        owned_kernel,
        out_shape=jax.ShapeDtypeStruct((RING, share * lanes + 8, 128), bf16),
        in_specs=[inside, inside, inside],
        out_specs=inside,
        name="owned",
    )(in_vmem(everyone), in_vmem(rows_hidden), in_vmem(kept_gain))

    near_rows = lax.all_to_all(piece, "ffn", 0, 0, tiled=True, axis_index_groups=near)
    pair_rows = lax.ppermute(near_rows, "ffn", pair)
    grad_hidden, grad_gain = pl.pallas_call(
        finish_kernel,
        out_shape=(jax.ShapeDtypeStruct((tokens, width), bf16), jax.ShapeDtypeStruct((lanes, 128), f32)),
        in_specs=[inside, inside],
        out_specs=(inside, inside),
        name="finish",
    )(in_vmem(near_rows), in_vmem(pair_rows))
    grad_gain = grad_gain.reshape(width)

    def weight_grad(lhs, rhs, dims):
        return lax.dot_general(lhs, rhs, (dims, ((), ())), preferred_element_type=f32).astype(bf16)

    grad_down = weight_grad(act_t, grad_out, ((1,), (0,)))
    grad_gate = weight_grad(scaled, gate_grad_t, ((0,), (1,)))
    grad_up = weight_grad(scaled, up_grad_t, ((0,), (1,)))
    return (grad_hidden, grad_gain, grad_gate, grad_up, grad_down)


def solution(mesh):
    placed = (P(None, "mp"), P("mp"), P(None, "mp"), P("mp", "ffn"), P("mp", "ffn"), P("ffn", "mp"))
    return jax.shard_map(
        body,
        mesh=mesh,
        in_specs=placed,
        out_specs=(P(None, "mp"), P("mp"), P("mp", "ffn"), P("mp", "ffn"), P("ffn", "mp")),
        check_vma=False,
    )
```

```python
import jax
import jax.numpy as jnp
from jax import lax
from jax.experimental import pallas as pl
from jax.experimental.pallas import tpu as pltpu
from jax.sharding import PartitionSpec as P

D = 8192
epsilon = 1e-05
RING = 4


def in_vmem(x):
    return pltpu.with_memory_space_constraint(x, pltpu.VMEM)


def place(tokens, share):
    me = lax.axis_index("ffn")
    core = lax.rem(me, 2)
    return core, core * (tokens // 2) + lax.rem(lax.div(me, 2), RING) * share


def split_terms(x):
    high = x.astype(jnp.bfloat16)
    return high, (x - high.astype(jnp.float32)).astype(jnp.bfloat16)


def across(lhs, rhs):
    return lax.dot_general(lhs, rhs, (((1,), (1,)), ((), ())), preferred_element_type=jnp.float32)


def partial_kernel(
    hidden_hbm,
    gain_ref,
    gate_hbm,
    up_hbm,
    grad_hbm,
    down_hbm,
    send_ref,
    gate,
    up,
    rows_ref,
    kept_gain,
    hidden,
    grad,
    down,
    sems,
):
    part = gate.shape[0] // 2
    pairs = [(hidden_hbm, hidden), (grad_hbm, grad)]
    for source, target in ((down_hbm, down), (gate_hbm, gate), (up_hbm, up)):
        for at in (0, part):
            pairs.append((source.at[pl.ds(at, part)], target.at[pl.ds(at, part)]))
    moves = [pltpu.make_async_copy(source, target, sems.at[i]) for i, (source, target) in enumerate(pairs)]
    for move in moves:
        move.start()
    pieces, rows, lanes = send_ref.shape
    units = gate.shape[0]
    ub = units * 2 // pieces

    def project(weight, acts, first, move):
        for n in range(2):
            moves[move + n].wait()
            sums = across(weight[n * part : (n + 1) * part], acts)
            for u in range(part // ub):
                for half in range(2):
                    send_ref[2 * (n * part // ub + u) + half, first : first + ub, :] = sums[
                        u * ub : (u + 1) * ub, half * lanes : (half + 1) * lanes
                    ].astype(jnp.bfloat16)

    moves[0].wait()
    wide = hidden[...].astype(jnp.float32)
    scaled = (wide * gain_ref[...]).astype(jnp.bfloat16)
    high, low = split_terms(wide * wide)
    ones = jnp.ones((8, hidden.shape[1]), jnp.bfloat16)
    squared = across(ones, high) + across(ones, low)
    high, low = split_terms(squared)
    row = lax.broadcasted_iota(jnp.int32, squared.shape, 0)
    extra = jnp.where(row == 0, high.astype(jnp.float32), jnp.where(row == 1, low.astype(jnp.float32), 0.0))
    for piece in range(pieces):
        half = piece % 2
        send_ref[piece, 3 * ub : rows, :] = extra[:, half * lanes : (half + 1) * lanes].astype(jnp.bfloat16)
    share = rows_ref.shape[1]
    first = pl.multiple_of(place(hidden.shape[0], share)[1], share)
    for l in range(rows_ref.shape[0]):
        rows_ref[l] = hidden[pl.ds(first, share), l * 128 : (l + 1) * 128].astype(jnp.float32)
    kept_gain[...] = gain_ref[...]
    moves[1].wait()
    project(down, grad[...], 2 * ub, 2)
    project(gate, scaled, 0, 4)
    project(up, scaled, ub, 6)


def partials(hidden_in, norm_gain, gate_rows, up_rows, grad_out, down_weight, pieces):
    tokens, width = hidden_in.shape
    units = gate_rows.shape[0]
    share = tokens // 2 // RING
    anywhere = pl.BlockSpec(memory_space=pl.ANY)
    inside = pl.BlockSpec(memory_space=pltpu.VMEM)
    return pl.pallas_call(
        partial_kernel,
        out_shape=(
            pltpu.VMEM((pieces, 3 * (units * 2 // pieces) + 8, tokens // 2), jnp.bfloat16),
            pltpu.VMEM((units, width), jnp.bfloat16),
            pltpu.VMEM((units, width), jnp.bfloat16),
            pltpu.VMEM((width // 128, share, 128), jnp.float32),
            pltpu.VMEM((1, width), jnp.float32),
        ),
        in_specs=[anywhere, inside, anywhere, anywhere, anywhere, anywhere],
        out_specs=(inside,) * 5,
        scratch_shapes=[
            pltpu.VMEM((tokens, width), jnp.bfloat16),
            pltpu.VMEM((tokens, width), jnp.bfloat16),
            pltpu.VMEM((units, width), jnp.bfloat16),
            pltpu.SemaphoreType.DMA((8,)),
        ],
        name="partials",
    )(hidden_in, norm_gain.reshape(1, width), gate_rows, up_rows, grad_out, down_weight)


def piece_kernel(came_ref, out_ref):
    pieces, rows, lanes = came_ref.shape
    ub = (rows - 8) // 3
    got = came_ref[0].astype(jnp.float32)
    for i in range(1, pieces):
        got = got + came_ref[i].astype(jnp.float32)
    square_sum = got[3 * ub : 3 * ub + 1] + got[3 * ub + 1 : 3 * ub + 2]
    inverse = lax.rsqrt(square_sum / D + epsilon)
    gate = inverse * got[:ub]
    up_val = inverse * got[ub : 2 * ub]
    act_grad = got[2 * ub : 3 * ub]
    sigma = jax.nn.sigmoid(gate)
    activation = (gate * sigma * up_val).astype(jnp.bfloat16)
    gate_grad = (inverse * act_grad * up_val * sigma * (1.0 + gate * (1.0 - sigma))).astype(jnp.bfloat16)
    up_grad = (inverse * act_grad * gate * sigma).astype(jnp.bfloat16)
    both = gate_grad.astype(jnp.float32) * gate + up_grad.astype(jnp.float32) * up_val
    pulled = jnp.broadcast_to(inverse * jnp.sum(both, axis=0, keepdims=True) / D, (8, lanes))
    high, low = split_terms(pulled)
    row = lax.broadcasted_iota(jnp.int32, (8, lanes), 0)
    extra = jnp.where(row == 0, high.astype(jnp.float32), jnp.where(row == 1, low.astype(jnp.float32), 0.0))
    extra = extra.astype(jnp.bfloat16)
    for i in range(pieces):
        out_ref[i, :ub, :] = activation
        out_ref[i, ub : 2 * ub, :] = gate_grad
        out_ref[i, 2 * ub : 3 * ub, :] = up_grad
        out_ref[i, 3 * ub :, :] = extra


def row_terms(pulled, used):
    high, low = split_terms(pulled)
    return (high.astype(jnp.float32) + pltpu.roll(low.astype(jnp.float32), used, 0)).astype(jnp.bfloat16)


def term_rows(terms, used):
    row = lax.broadcasted_iota(jnp.int32, (8, 128), 0)
    return jnp.where(row < used, terms + pltpu.roll(terms, 8 - used, 0), 0.0)


def other_kernel(gate_ref, up_ref, all_ref, out_ref, part_ref, pulled_ref, gate_grad, up_grad):
    tokens, width = part_ref.shape
    half, lanes = tokens // 2, width // 128
    pieces, rows, _ = all_ref.shape
    ub = (rows - 8) // 3
    for i in range(pieces):
        u, h = i // 2, i % 2
        gate_grad[u * ub : (u + 1) * ub, h * half : (h + 1) * half] = all_ref[i, ub : 2 * ub]
        up_grad[u * ub : (u + 1) * ub, h * half : (h + 1) * half] = all_ref[i, 2 * ub : 3 * ub]

    def down_first(lhs, rhs):
        return lax.dot_general(lhs, rhs, (((0,), (0,)), ((), ())), preferred_element_type=jnp.float32)

    part_ref[...] = down_first(gate_grad[...], gate_ref[...]) + down_first(up_grad[...], up_ref[...])
    base = pl.multiple_of((1 - place(tokens, 1)[0]) * half, half)
    for l in range(lanes):
        out_ref[l * half : (l + 1) * half] = part_ref[pl.ds(base, half), l * 128 : (l + 1) * 128].astype(jnp.bfloat16)
    row = lax.broadcasted_iota(jnp.int32, (8, 128), 0)
    pulled = jnp.zeros((8, 128), jnp.float32)
    for h in range(2):
        got = all_ref[h, rows - 8 :].astype(jnp.float32)
        for i in range(2 + h, pieces, 2):
            got = got + all_ref[i, rows - 8 :].astype(jnp.float32)
        pulled = jnp.where(row == h, got[0:1] + got[1:2], pulled)
    pulled_ref[...] = pulled
    out_ref[lanes * half :] = row_terms(pulled, tokens // 128)


def added_kernel(came_ref, out_ref):
    total = came_ref[0].astype(jnp.float32)
    for k in range(1, came_ref.shape[0]):
        total = total + came_ref[k].astype(jnp.float32)
    rows = total.shape[0] - 8
    out_ref[:rows] = total[:rows].astype(jnp.bfloat16)
    out_ref[rows:] = row_terms(term_rows(total[rows:], 2), 2)


def cuts_kernel(part_ref, came_ref, pulled_ref, out_ref):
    ring = out_ref.shape[0]
    tokens, width = part_ref.shape
    half, lanes = tokens // 2, width // 128
    share = half // ring
    base = place(tokens, share)[0] * half
    for k in range(ring):
        at = pl.multiple_of(base + k * share, share)
        for l in range(lanes):
            other = came_ref[l * half + k * share : l * half + (k + 1) * share].astype(jnp.float32)
            total = part_ref[pl.ds(at, share), l * 128 : (l + 1) * 128] + other
            out_ref[k, l * share : (l + 1) * share] = total.astype(jnp.bfloat16)
    used = tokens // 128
    pulled = pulled_ref[...] + term_rows(came_ref[half * lanes :].astype(jnp.float32), used)
    extra = row_terms(pulled, used)
    for k in range(ring):
        out_ref[k, lanes * share :] = extra


def owned_kernel(all_ref, hidden_ref, gain_ref, out_ref):
    lanes, share, _ = hidden_ref.shape
    total = all_ref[0].astype(jnp.float32)
    for i in range(1, all_ref.shape[0]):
        total = total + all_ref[i].astype(jnp.float32)
    core, first = place(share * RING * 2, share)
    pulled = term_rows(total[lanes * share :], 2)
    pulled = jnp.where(core == 0, pulled[0:1], pulled[1:2])
    row = lax.broadcasted_iota(jnp.int32, (share, 128), 0)
    lane = lax.broadcasted_iota(jnp.int32, (share, 128), 1)
    here = lane == row + (first - core * 128)
    pulled = jnp.sum(jnp.where(here, jnp.broadcast_to(pulled, (share, 128)), 0.0), axis=1, keepdims=True)
    row = lax.broadcasted_iota(jnp.int32, (8, 128), 0)
    extra = jnp.zeros((8, 128), jnp.float32)
    for l in range(lanes):
        grad = total[l * share : (l + 1) * share]
        wide = hidden_ref[l]
        rows = (gain_ref[:, l * 128 : (l + 1) * 128] * grad - wide * pulled).astype(jnp.bfloat16)
        high, low = split_terms(jnp.broadcast_to(jnp.sum(wide * grad, axis=0, keepdims=True), (8, 128)))
        extra = jnp.where(row == l, high.astype(jnp.float32), extra)
        extra = jnp.where(row == lanes + l, low.astype(jnp.float32), extra)
        for k in range(out_ref.shape[0]):
            out_ref[k, l * share : (l + 1) * share] = rows
    for k in range(out_ref.shape[0]):
        out_ref[k, lanes * share :] = extra.astype(jnp.bfloat16)


def finish_kernel(near_ref, pair_ref, rows_ref, gain_ref):
    ring, rows, lane = near_ref.shape
    lanes = rows_ref.shape[1] // lane
    share = (rows - 2 * lanes) // lanes
    first = place(rows_ref.shape[0], share)[0] == 0
    total = jnp.zeros((lanes, lane), jnp.float32)
    for half in range(2):
        take_near = first if half == 0 else jnp.logical_not(first)
        for k in range(ring):
            got = jnp.where(take_near, near_ref[k].astype(jnp.float32), pair_ref[k].astype(jnp.float32))
            at = (half * ring + k) * share
            for l in range(lanes):
                rows_ref[at : at + share, l * lane : (l + 1) * lane] = got[l * share : (l + 1) * share].astype(jnp.bfloat16)
            total = total + (got[lanes * share : lanes * share + lanes] + got[lanes * share + lanes :])
    gain_ref[...] = total


def body(hidden_in, norm_gain, grad_out, gate_weight, up_weight, down_weight):
    f32, bf16 = jnp.float32, jnp.bfloat16
    tokens, width = hidden_in.shape
    units = gate_weight.shape[1]
    mp, ffn = lax.axis_size("mp"), lax.axis_size("ffn")
    ublocks, thalf = mp // 2, tokens // 2
    ub = units // ublocks
    levels = ffn // 2 // RING
    send, gate_rows, up_rows, rows_hidden, kept_gain = partials(
        hidden_in, norm_gain, gate_weight.T, up_weight.T, grad_out, down_weight, mp
    )
    scaled = (hidden_in.astype(f32) * norm_gain).astype(bf16)
    came = lax.all_to_all(send, "mp", 0, 0, tiled=True)
    piece = pl.pallas_call(
        piece_kernel, out_shape=pltpu.VMEM(came.shape, bf16), name="piece"
    )(in_vmem(came))
    everything_flat = lax.all_to_all(piece, "mp", 0, 0, tiled=True)
    everything = everything_flat.reshape(ublocks, 2, 3 * ub + 8, thalf)

    def joined(k):
        part = everything[:, :, k * ub : (k + 1) * ub]
        return part.transpose(0, 2, 1, 3).reshape(units, tokens)

    act_t, gate_grad_t, up_grad_t = joined(0), joined(1), joined(2)
    lanes = width // 128
    inside = pl.BlockSpec(memory_space=pltpu.VMEM)
    packed, input_part, pulled = pl.pallas_call(
        other_kernel,
        out_shape=(
            pltpu.VMEM((thalf * lanes + 8, 128), bf16),
            pltpu.VMEM((tokens, width), f32),
            pltpu.VMEM((8, 128), f32),
        ),
        scratch_shapes=[pltpu.VMEM((units, tokens), bf16), pltpu.VMEM((units, tokens), bf16)],
        name="other",
    )(in_vmem(gate_rows), in_vmem(up_rows), in_vmem(everything_flat))
    pair = [(i, i ^ 1) for i in range(ffn)]
    came = lax.ppermute(packed, "ffn", pair)
    share = thalf // RING
    near = [[(g * RING + j) * 2 + c for j in range(RING)] for g in range(levels) for c in range(2)]
    cuts = pl.pallas_call(
        cuts_kernel,
        out_shape=pltpu.VMEM((RING, share * lanes + 8, 128), bf16),
        in_specs=[inside, inside, inside],
        out_specs=inside,
        name="cuts",
    )(in_vmem(input_part), in_vmem(came), in_vmem(pulled))
    came = lax.all_to_all(cuts, "ffn", 0, 0, tiled=True, axis_index_groups=near)

    packed = pl.pallas_call(
        added_kernel, out_shape=pltpu.VMEM(came.shape[1:], bf16), name="added"
    )(in_vmem(came))
    owners = [[(k * RING + j) * 2 + c for k in range(levels)] for j in range(RING) for c in range(2)]
    everyone = lax.all_gather(packed, "ffn", axis_index_groups=owners)
    piece = pl.pallas_call(
        owned_kernel,
        out_shape=jax.ShapeDtypeStruct((RING, share * lanes + 8, 128), bf16),
        in_specs=[inside, inside, inside],
        out_specs=inside,
        name="owned",
    )(in_vmem(everyone), in_vmem(rows_hidden), in_vmem(kept_gain))

    near_rows = lax.all_to_all(piece, "ffn", 0, 0, tiled=True, axis_index_groups=near)
    pair_rows = lax.ppermute(near_rows, "ffn", pair)
    grad_hidden, grad_gain = pl.pallas_call(
        finish_kernel,
        out_shape=(jax.ShapeDtypeStruct((tokens, width), bf16), jax.ShapeDtypeStruct((lanes, 128), f32)),
        in_specs=[inside, inside],
        out_specs=(inside, inside),
        name="finish",
    )(in_vmem(near_rows), in_vmem(pair_rows))
    grad_gain = grad_gain.reshape(width)

    def weight_grad(lhs, rhs, dims):
        return lax.dot_general(lhs, rhs, (dims, ((), ())), preferred_element_type=f32).astype(bf16)

    grad_down = weight_grad(act_t, grad_out, ((1,), (0,)))
    grad_gate = weight_grad(scaled, gate_grad_t, ((0,), (1,)))
    grad_up = weight_grad(scaled, up_grad_t, ((0,), (1,)))
    return (grad_hidden, grad_gain, grad_gate, grad_up, grad_down)


def solution(mesh):
    placed = (P(None, "mp"), P("mp"), P(None, "mp"), P("mp", "ffn"), P("mp", "ffn"), P("ffn", "mp"))
    return jax.shard_map(
        body,
        mesh=mesh,
        in_specs=placed,
        out_specs=(P(None, "mp"), P("mp"), P("mp", "ffn"), P("mp", "ffn"), P("ffn", "mp")),
        check_vma=False,
    )
```
